32 devices in a mesh: blk: 16 (over z, y, core), grp: 2 (over x).
Axes of the slice: x: 2, y: 2, z: 4, core: 2. Of those that a mesh axis runs over, the one named last changes fastest.
Arguments:
- points: float32 [4096, 4096], P(('blk', 'grp')), may hold values from -40 to 40
- cand_index: int32 [32, 128], P(('blk', 'grp')), may hold values from 0 to 127, as said below
- cand_count: int32 [32], P(('blk', 'grp')), may hold values from 32 to 128
- neighbor_ids: int32 [4096, 16], P(('blk', 'grp')), may hold values from 0 to 4095
- old_dist: float32 [4096, 16], P(('blk', 'grp')), may hold values from 0.3 to 10
Outputs:
- scaled_dist: float32 [4096, 16], P(('blk', 'grp'))
The draws below stay inside these ranges and needn't reach their ends.
Inputs may be any that keep to these rules, and one draw needn't show every extreme that they name: `cand_index`: within each row, distinct indices of rows of the block.
All inputs are finite; a program needn't handle non-finite values.
Results may differ from the reference program's by a relative error of at most 0.0003.
Values sent between devices are 32-bit elements; how exact they have to be, the bound alone decides.
No kernel may reach another device: no remote copies, remote signals or barrier semaphores. Data moves between devices by JAX's collectives and lax.ppermute only.
A program may use at most 128 MiB of HBM per device.

```python
import math
import jax
import jax.numpy as jnp
from jax import lax

D = 4096
KNN = 16
CAND = 128
REACH = 2
PTS_DEV = 128
BLOCKS = 32
NPTS = 4096
N_BLK = 16
N_GRP = 2


def draw_points(key, part):
    keys = jax.random.split(jax.random.fold_in(key, 11), 6)
    clusters = max(2, (2 * REACH + 1) * N_GRP * CAND // (3 * KNN))
    position = jnp.arange(NPTS, dtype=jnp.float32) / NPTS
    trend = jnp.exp(0.5 * math.log(3.0) * position)
    member = jax.random.randint(keys[0], (NPTS,), 0, clusters, jnp.int32)
    centre_scale = jnp.exp(jax.random.uniform(keys[1], (clusters, 1), jnp.float32, 0.0, math.log(3.0)))
    centres = jnp.clip(jax.random.normal(keys[2], (clusters, D), jnp.float32), -4.0, 4.0)
    noise = jnp.clip(jax.random.normal(keys[4], (NPTS, D), jnp.float32), -4.0, 4.0)
    jitter = jnp.exp(jax.random.uniform(keys[5], (NPTS, 1), jnp.float32, 0.0, 0.5 * math.log(10.0)))
    placed = (centres * centre_scale)[member]
    value = placed + 0.35 * jitter * noise
    return value * trend[:, None]


def first_rows(subkey):
    return jax.random.permutation(subkey, PTS_DEV)[:CAND].astype(jnp.int32)


def draw_cand_index(key, part):
    subkeys = jax.random.split(jax.random.fold_in(key, 23), BLOCKS)
    return jax.vmap(first_rows)(subkeys)


def draw_neighbor_ids(key, part):
    first, second, third = jax.random.split(jax.random.fold_in(key, 37), 3)
    row_block = jnp.arange(NPTS, dtype=jnp.int32) // PTS_DEV
    cycle_pos = row_block // N_GRP
    offset = jax.random.randint(first, (NPTS, KNN), -REACH, REACH + 1, jnp.int32)
    member = jax.random.randint(second, (NPTS, KNN), 0, N_GRP, jnp.int32)
    within = jax.random.randint(third, (NPTS, KNN), 0, PTS_DEV, jnp.int32)
    source = (cycle_pos[:, None] + offset) % N_BLK * N_GRP + member
    return (source * PTS_DEV + within).astype(jnp.int32)


def touch_ends(result, rng, low, high):
    index_at = [jax.random.randint(jax.random.fold_in(rng, axis), (), 0, length) for axis, length in enumerate(result.shape)]
    widest = result.shape.index(max(result.shape))
    neighbour = index_at[:widest] + [(index_at[widest] + 1) % result.shape[widest]] + index_at[widest + 1:]
    return result.at[tuple(index_at)].set(low).at[tuple(neighbour)].set(high)


def level_of(stream_key, shape, cuts, low, top_value):
    def one(axis_at, blocks):
        draws = jax.random.uniform(jax.random.fold_in(jax.random.fold_in(stream_key, 6), axis_at), (blocks,), jnp.float32, low / len(cuts), top_value / len(cuts))
        return jnp.repeat(jnp.exp(draws), shape[axis_at] // blocks).reshape((-1,) + (1,) * (len(shape) - axis_at - 1))

    level = one(*cuts[0])
    for cut in cuts[1:]:
        level = level * one(*cut)
    return level


def setup_inputs(seed: int = 0) -> dict:
    splits = jax.random.split(jax.random.key(seed), 6)
    points = draw_points(jax.random.fold_in(splits[5], 71), 0)
    cand_index = draw_cand_index(jax.random.fold_in(splits[5], 71), 0)
    cand_count = touch_ends(jax.random.randint(splits[2], (BLOCKS,), CAND // 4, CAND + 1), jax.random.fold_in(splits[2], 1), CAND // 4, CAND).astype(jnp.int32)
    neighbor_ids = draw_neighbor_ids(jax.random.fold_in(splits[5], 71), 0)
    old_dist = jnp.clip(jnp.exp(math.log(10.0) - 3.506558 * jax.random.uniform(splits[4], (NPTS, KNN), jnp.float32) ** level_of(splits[4], (NPTS, KNN), ((0, 32),), -0.2, 0.2)), 0.3, 10.0)
    return dict(points=points, cand_index=cand_index, cand_count=cand_count, neighbor_ids=neighbor_ids, old_dist=old_dist)


far_value = 1e30


def pick_rows(block_points, block_index):
    return block_points[block_index]


def reference(points, cand_index, cand_count, neighbor_ids, old_dist):
    blocks = N_BLK * N_GRP
    grouped = points.reshape(blocks, PTS_DEV, D)
    slots = jnp.arange(CAND, dtype=jnp.int32)
    anchor = jnp.arange(blocks, dtype=jnp.int32)
    cand_ids = jnp.where(slots[None, :] < cand_count[:, None], anchor[:, None] * PTS_DEV + cand_index, -1).astype(jnp.int32)
    cand_rows = jax.vmap(pick_rows)(grouped, cand_index)
    cand_norms = jnp.sum(cand_rows * cand_rows, axis=2)
    offsets = jnp.arange(-REACH, REACH + 1, dtype=jnp.int32)
    members = jnp.arange(N_GRP, dtype=jnp.int32)
    lists = neighbor_ids.reshape(blocks, PTS_DEV, KNN)
    stored = old_dist.reshape(blocks, PTS_DEV, KNN)

    def one_block(block):
        cycle_pos = block // N_GRP
        sources = (((cycle_pos + offsets) % N_BLK)[:, None] * N_GRP + members[None, :]).reshape(-1)
        rows = cand_rows[sources].reshape(-1, D)
        row_ids = cand_ids[sources].reshape(-1)
        row_norms = cand_norms[sources].reshape(-1)
        local = grouped[block]
        local_norms = jnp.sum(local * local, axis=1)
        inner = jnp.dot(local, rows.T, precision=lax.Precision.HIGHEST, preferred_element_type=jnp.float32)
        distance = (local_norms[:, None] + row_norms[None, :] - 2.0 * inner) / D
        own_ids = block * PTS_DEV + jnp.arange(PTS_DEV, dtype=jnp.int32)
        known = jnp.any(lists[block][:, :, None] == row_ids[None, None, :], axis=1)
        masked = (row_ids[None, :] < 0) | (row_ids[None, :] == own_ids[:, None]) | known
        distance = jnp.where(masked, jnp.float32(far_value), distance)
        joined = jnp.concatenate([stored[block], distance], axis=1)
        return jnp.sort(joined, axis=1)[:, :KNN]

    best = lax.map(one_block, jnp.arange(blocks, dtype=jnp.int32)).reshape(NPTS, KNN)
    mean_last = jnp.sum(best[:, KNN - 1]) / NPTS
    return best / mean_last
```

```python
import functools

import jax
import jax.numpy as jnp
from jax import lax
from jax.experimental import pallas as pl
from jax.experimental.pallas import tpu as pltpu
from jax.sharding import PartitionSpec as P

AXES = ("blk", "grp")
LANES = 128
SUBLANES = 8
NT = (((1,), (1,)), ((), ()))
FAR = 1e30
NEVER = -3e38


def exchange(tiles, i, j):
    low, high = jnp.minimum(tiles[i], tiles[j]), jnp.maximum(tiles[i], tiles[j])
    tiles[i], tiles[j] = low, high


def sort_tiles(tiles):
    tiles = list(tiles)
    n = len(tiles)
    p = 1
    while p < n:
        k = p
        while k >= 1:
            for j in range(k % p, n - k, 2 * k):
                for i in range(min(k, n - j - k)):
                    if (i + j) // (2 * p) == (i + j + k) // (2 * p):
                        exchange(tiles, i + j, i + j + k)
            k //= 2
        p *= 2
    return tiles


def bitonic(tiles):
    tiles = list(tiles)
    step = len(tiles) // 2
    while step >= 1:
        for i in range(len(tiles)):
            if not i & step:
                exchange(tiles, i, i + step)
        step //= 2
    return tiles


def merge_lowest(a, b, keep):
    if len(a) + len(b) <= keep:
        return bitonic(a + b[::-1])
    return bitonic([jnp.minimum(x, y) for x, y in zip(a, b[::-1])])


def lowest(tiles, keep):
    group = 1
    while group * 2 <= min(keep, len(tiles)):
        group *= 2
    while len(tiles) % group:
        tiles = tiles + [jnp.full((SUBLANES, LANES), FAR, jnp.float32)]
    lists = [sort_tiles(tiles[i : i + group]) for i in range(0, len(tiles), group)]
    while len(lists) > 1:
        paired = [
            merge_lowest(lists[i], lists[i + 1], keep)
            for i in range(0, len(lists) - 1, 2)
        ]
        if len(lists) % 2:
            rest = lists[-1]
            while len(rest) < len(paired[0]):
                rest = rest + [jnp.full((SUBLANES, LANES), FAR, jnp.float32)]
            paired.append(rest)
        lists = paired
    found = lists[0]
    shift = SUBLANES // 2
    while shift:
        found = merge_lowest(found, [pltpu.roll(t, shift, 0) for t in found], keep)
        shift //= 2
    return found


def tiles_of(array):
    return [array[i : i + SUBLANES] for i in range(0, array.shape[0], SUBLANES)]


def describe_kernel(count_ref, index_ref, lists_ref, meta_ref):
    pts = lists_ref.shape[0]
    listed = lists_ref.shape[1]
    slots = index_ref.shape[1]
    wide = jnp.concatenate(
        [
            lists_ref[...].astype(jnp.float32),
            jnp.zeros((pts, LANES - listed), jnp.float32),
        ],
        axis=1,
    )
    meta_ref[0:listed] = wide.T[:listed].astype(jnp.int32)
    spread = jnp.broadcast_to(index_ref[...].astype(jnp.float32), (pts, slots)).T
    slot = lax.broadcasted_iota(jnp.int32, (slots, pts), 0)
    row = lax.broadcasted_iota(jnp.int32, (slots, pts), 1)
    hit = (spread.astype(jnp.int32) == row) & (slot < count_ref[0])
    live = jnp.max(jnp.where(hit, 1.0, 0.0), axis=0, keepdims=True)
    meta_ref[listed : listed + SUBLANES] = jnp.broadcast_to(
        live.astype(jnp.int32), (SUBLANES, pts)
    )


def mask_kernel(listed, base_ref, o, t, o2, t2, u, v, own_ref, far_ref):
    metas = (o, t, o2, t2, u, v)
    pts = o.shape[1]
    alive = [
        jnp.broadcast_to(m[listed : listed + 1].astype(jnp.float32), (pts, pts)).T > 0.5
        for m in metas
    ]
    row = lax.broadcasted_iota(jnp.int32, (pts, pts), 0)
    lane = lax.broadcasted_iota(jnp.int32, (pts, pts), 1)

    def floor(target, cand):
        ids = row + base_ref[cand] * pts
        lists = metas[target]
        bad = jnp.logical_not(alive[cand])
        for k in range(listed):
            bad = bad | (ids == lists[k : k + 1])
        if target == cand:
            bad = bad | (row == lane)
        return jnp.where(bad, FAR, NEVER)

    for i in range(6):
        own_ref[i * pts : (i + 1) * pts] = floor(0, i)
    for i, (target, cand) in enumerate(((2, 4), (2, 5), (4, 0), (4, 2))):
        far_ref[i * pts : (i + 1) * pts] = floor(target, cand)


def partial_kernel(o, t, o2, t2, u, v, mine_ref, sib_ref, hi, lo, near, far, squares):
    step = pl.program_id(0)
    pts = o.shape[0]

    @pl.when(step == 0)
    def _():
        near[...] = jnp.zeros_like(near)
        far[...] = jnp.zeros_like(far)
        squares[...] = jnp.zeros_like(squares)

    for i, ref in enumerate((o, t, o2, t2, u, v)):
        at = slice(i * pts, (i + 1) * pts)
        x = ref[...]
        high = x.astype(jnp.bfloat16)
        hi[at] = high
        lo[at] = (x - high.astype(jnp.float32)).astype(jnp.bfloat16)
        total = squares[at]
        for j in range(0, x.shape[1], LANES):
            part = x[:, j : j + LANES]
            total = total + part * part
        squares[at] = total

    def dot(a, b):
        return lax.dot_general(a, b, NT, preferred_element_type=jnp.float32)

    def product(rows, columns):
        return (
            dot(hi[rows], lo[columns])
            + dot(lo[rows], hi[columns])
            + dot(hi[rows], hi[columns])
        )

    near[...] += product(slice(0, 6 * pts), slice(0, 2 * pts))
    far[...] += product(slice(4 * pts, 6 * pts), slice(2 * pts, 4 * pts))

    @pl.when(step == pl.num_programs(0) - 1)
    def _():
        down = jnp.sum(squares[...], axis=1, keepdims=True)
        across = [
            jnp.sum(squares[i * pts : (i + 1) * pts].T, axis=0, keepdims=True)
            for i in range(4)
        ]

        def put(ref, at, source, cand, offset, target):
            rows = slice((cand - offset) * pts, (cand - offset + 1) * pts)
            lanes = slice((target % 2) * pts, (target % 2 + 1) * pts)
            ref[at * pts : (at + 1) * pts] = (
                down[cand * pts : (cand + 1) * pts]
                + across[target]
                - 2.0 * source[rows, lanes]
            )

        for i in range(6):
            put(mine_ref, i, near, i, 0, 0)
            put(sib_ref, i, near, i ^ 1, 0, 1)
        for i in range(2):
            put(mine_ref, 6 + i, far, 4 + i, 4, 2)
            put(sib_ref, 6 + i, far, 5 - i, 4, 3)


def exchange_kernel(scale, keep, mine, theirs, floors, across_ref, along_ref):
    pts = mine.shape[1]

    def whole(i):
        at = slice(i * pts, (i + 1) * pts)
        return (mine[at] + theirs[at]) * scale

    def store(ref, blocks):
        tiles = []
        for i, block in blocks:
            tiles += tiles_of(jnp.maximum(block, floors[i * pts : (i + 1) * pts]))
        for i, tile in enumerate(lowest(tiles, keep)):
            ref[i : i + 1] = tile[0:1]

    store(across_ref, ((0, whole(6)), (1, whole(7))))
    store(along_ref, ((2, whole(4).T), (3, whole(6).T)))


def own_kernel(scale, keep, mine, theirs, floors, old, found_ref):
    pts = mine.shape[1]
    tiles = []
    for i in range(6):
        at = slice(i * pts, (i + 1) * pts)
        tiles += tiles_of(jnp.maximum((mine[at] + theirs[at]) * scale, floors[at]))
    for i, tile in enumerate(lowest(tiles, keep)):
        found_ref[i : i + 1] = tile[0:1]
    wide = jnp.concatenate(
        [old[...], jnp.zeros((pts, LANES - keep), jnp.float32)], axis=1
    )
    found_ref[keep : 2 * keep] = wide.T[:keep]


def finish_kernel(keep, found, across, along, best_ref, total_ref):
    tiles = tiles_of(found[...]) + tiles_of(across[...]) + tiles_of(along[...])
    ranked = lowest(tiles, keep)
    total_ref[...] = jnp.broadcast_to(
        jnp.sum(ranked[keep - 1], axis=1, keepdims=True), total_ref.shape
    )
    rows = jnp.concatenate(
        [tile[0:1] for tile in ranked]
        + [jnp.zeros((LANES - keep, LANES), jnp.float32)],
        axis=0,
    )
    best_ref[...] = rows.T[:, :keep]


def body(points, cand_index, cand_count, neighbor_ids, old_dist):
    pts, width = points.shape
    keep = old_dist.shape[1]
    cycle = lax.axis_size("blk")
    members = lax.axis_size("grp")
    half = width // 2
    blk = lax.axis_index("blk")
    grp = lax.axis_index("grp")
    core = blk % 2
    f32 = jnp.float32

    def links(move):
        return [
            (b * members + g, (move(b, g)[0] % cycle) * members + move(b, g)[1])
            for b in range(cycle)
            for g in range(members)
        ]

    sibling = links(lambda b, g: (b ^ 1, g))
    over_same = links(lambda b, g: (b, 1 - g))
    over_cross = links(lambda b, g: (b ^ 1, 1 - g))
    along_same = links(lambda b, g: (b + (2 if b % 2 else -2), g))
    along_cross = links(lambda b, g: (b + (1 if b % 2 else -1), g))
    along_back = [(b, a) for a, b in along_same]

    def send(array, pairs):
        return lax.ppermute(array, AXES, pairs)

    o = lax.dynamic_slice(points, (0, core * half), (pts, half))
    other = lax.dynamic_slice(points, (0, (1 - core) * half), (pts, half))
    o2 = send(o, over_same)
    u = send(o, along_same)
    t2 = send(other, over_cross)
    v = send(other, along_cross)
    t = send(other, sibling)

    whole_array = pl.BlockSpec(memory_space=pltpu.VMEM)
    scalars = pl.BlockSpec(memory_space=pltpu.SMEM)
    meta = pl.pallas_call(
        describe_kernel,
        out_shape=jax.ShapeDtypeStruct((keep + SUBLANES, pts), jnp.int32),
        in_specs=[scalars, whole_array, whole_array],
        out_specs=whole_array,
    )(cand_count, cand_index, neighbor_ids)
    metas = (
        meta,
        send(meta, sibling),
        send(meta, over_same),
        send(meta, over_cross),
        send(meta, along_same),
        send(meta, along_cross),
    )
    ahead = jnp.where(core == 0, 2, -2)
    beside = jnp.where(core == 0, -1, 1)
    steps = (0, 1 - 2 * core, 0, 1 - 2 * core, ahead, beside)
    sides = (grp, grp, 1 - grp, 1 - grp, grp, grp)
    bases = jnp.stack(
        [
            ((blk + step + cycle) % cycle) * members + side
            for step, side in zip(steps, sides)
        ]
    ).astype(jnp.int32)
    own_floor, far_floor = pl.pallas_call(
        functools.partial(mask_kernel, keep),
        out_shape=(
            jax.ShapeDtypeStruct((6 * pts, pts), f32),
            jax.ShapeDtypeStruct((4 * pts, pts), f32),
        ),
        in_specs=[scalars] + [whole_array] * 6,
        out_specs=(whole_array, whole_array),
    )(bases, *metas)

    tile = min(half, 512)
    cut = pl.BlockSpec((pts, tile), lambda i: (0, i))
    result = pl.BlockSpec((8 * pts, pts), lambda i: (0, 0))
    mine, for_sibling = pl.pallas_call(
        partial_kernel,
        grid=(half // tile,),
        out_shape=(jax.ShapeDtypeStruct((8 * pts, pts), f32),) * 2,
        in_specs=[cut] * 6,
        out_specs=(result, result),
        scratch_shapes=[
            pltpu.VMEM((6 * pts, tile), jnp.bfloat16),
            pltpu.VMEM((6 * pts, tile), jnp.bfloat16),
            pltpu.VMEM((6 * pts, 2 * pts), f32),
            pltpu.VMEM((2 * pts, 2 * pts), f32),
            pltpu.VMEM((6 * pts, LANES), f32),
        ],
    )(o, t, o2, t2, u, v)
    theirs = send(for_sibling, sibling)

    scale = 1.0 / width
    across, along = pl.pallas_call(
        functools.partial(exchange_kernel, scale, keep),
        out_shape=(jax.ShapeDtypeStruct((keep, pts), f32),) * 2,
        in_specs=[whole_array] * 3,
        out_specs=(whole_array,) * 2,
    )(mine, theirs, far_floor)
    across = send(across, over_same)
    along = send(along, along_back)
    found = pl.pallas_call(
        functools.partial(own_kernel, scale, keep),
        out_shape=jax.ShapeDtypeStruct((2 * keep, pts), f32),
        in_specs=[whole_array] * 4,
        out_specs=whole_array,
    )(mine, theirs, own_floor, old_dist)
    best, total = pl.pallas_call(
        functools.partial(finish_kernel, keep),
        out_shape=(
            jax.ShapeDtypeStruct((pts, keep), f32),
            jax.ShapeDtypeStruct((SUBLANES, LANES), f32),
        ),
        in_specs=[whole_array] * 3,
        out_specs=(whole_array,) * 2,
    )(found, across, along)

    total = total + send(total, over_same)
    if cycle & (cycle - 1):
        total = lax.psum(total, "blk")
    else:
        bit = 1
        while bit < cycle:
            total = total + send(total, links(lambda b, g: (b ^ bit, g)))
            bit *= 2
    mean_last = total[0, 0] / (pts * cycle * members)
    return best / mean_last


def solution(mesh):
    return jax.shard_map(
        body,
        mesh=mesh,
        in_specs=(
            P(AXES, None),
            P(AXES, None),
            P(AXES),
            P(AXES, None),
            P(AXES, None),
        ),
        out_specs=P(AXES, None),
        check_vma=False,
    )
```

```python
import functools

import jax
import jax.numpy as jnp
from jax import lax
from jax.experimental import pallas as pl
from jax.experimental.pallas import tpu as pltpu
from jax.sharding import PartitionSpec as P


AXES = ("blk", "grp")
LANES = 128
SUBLANES = 8
NT = (((1,), (1,)), ((), ()))
FAR = 1e30
NEVER = -3e38


def exchange(tiles, i, j):
    low, high = jnp.minimum(tiles[i], tiles[j]), jnp.maximum(tiles[i], tiles[j])
    tiles[i], tiles[j] = low, high


def sort_tiles(tiles):
    tiles = list(tiles)
    n = len(tiles)
    p = 1
    while p < n:
        k = p
        while k >= 1:
            for j in range(k % p, n - k, 2 * k):
                for i in range(min(k, n - j - k)):
                    if (i + j) // (2 * p) == (i + j + k) // (2 * p):
                        exchange(tiles, i + j, i + j + k)
            k //= 2
        p *= 2
    return tiles


def bitonic(tiles):
    tiles = list(tiles)
    step = len(tiles) // 2
    while step >= 1:
        for i in range(len(tiles)):
            if not i & step:
                exchange(tiles, i, i + step)
        step //= 2
    return tiles


def merge_lowest(a, b, keep):
    if len(a) + len(b) <= keep:
        return bitonic(a + b[::-1])
    return bitonic([jnp.minimum(x, y) for x, y in zip(a, b[::-1])])


def lowest(tiles, keep):
    group = 1
    while group * 2 <= min(keep, len(tiles)):
        group *= 2
    while len(tiles) % group:
        tiles = tiles + [jnp.full((SUBLANES, LANES), FAR, jnp.float32)]
    lists = [sort_tiles(tiles[i : i + group]) for i in range(0, len(tiles), group)]
    while len(lists) > 1:
        paired = [
            merge_lowest(lists[i], lists[i + 1], keep)
            for i in range(0, len(lists) - 1, 2)
        ]
        if len(lists) % 2:
            rest = lists[-1]
            while len(rest) < len(paired[0]):
                rest = rest + [jnp.full((SUBLANES, LANES), FAR, jnp.float32)]
            paired.append(rest)
        lists = paired
    found = lists[0]
    shift = SUBLANES // 2
    while shift:
        found = merge_lowest(found, [pltpu.roll(t, shift, 0) for t in found], keep)
        shift //= 2
    return found


def tiles_of(array):
    return [array[i : i + SUBLANES] for i in range(0, array.shape[0], SUBLANES)]


def describe_kernel(count_ref, index_ref, lists_ref, meta_ref):
    listed, pts = lists_ref.shape
    slots = index_ref.shape[1]
    meta_ref[0:listed] = lists_ref[...]
    spread = jnp.broadcast_to(index_ref[...].astype(jnp.float32), (pts, slots)).T
    slot = lax.broadcasted_iota(jnp.int32, (slots, pts), 0)
    row = lax.broadcasted_iota(jnp.int32, (slots, pts), 1)
    hit = (spread.astype(jnp.int32) == row) & (slot < count_ref[0])
    live = jnp.max(jnp.where(hit, 1.0, 0.0), axis=0, keepdims=True)
    meta_ref[listed : listed + SUBLANES] = jnp.broadcast_to(
        live.astype(jnp.int32), (SUBLANES, pts)
    )


def mask_kernel(listed, base_ref, o, t, o2, t2, u, v, own_ref, far_ref):
    metas = (o, t, o2, t2, u, v)
    pts = o.shape[1]
    alive = [
        jnp.broadcast_to(m[listed : listed + 1].astype(jnp.float32), (pts, pts)).T > 0.5
        for m in metas
    ]
    row = lax.broadcasted_iota(jnp.int32, (pts, pts), 0)
    lane = lax.broadcasted_iota(jnp.int32, (pts, pts), 1)

    def floor(target, cand):
        ids = row + base_ref[cand] * pts
        lists = metas[target]
        bad = jnp.logical_not(alive[cand])
        for k in range(listed):
            bad = bad | (ids == lists[k : k + 1])
        if target == cand:
            bad = bad | (row == lane)
        return jnp.where(bad, FAR, NEVER)

    for i in range(6):
        own_ref[i * pts : (i + 1) * pts] = floor(0, i)
    for i, (target, cand) in enumerate(((2, 4), (2, 5), (4, 0), (4, 2))):
        far_ref[i * pts : (i + 1) * pts] = floor(target, cand)


def split(x):
    high = x.astype(jnp.bfloat16)
    return high, (x - high.astype(jnp.float32)).astype(jnp.bfloat16)


def squared(x):
    total = x[:, :LANES] * x[:, :LANES]
    for j in range(LANES, x.shape[1], LANES):
        total = total + x[:, j : j + LANES] * x[:, j : j + LANES]
    return total


def product(rows, columns):
    def dot(a, b):
        return lax.dot_general(a, b, NT, preferred_element_type=jnp.float32)

    return (
        dot(rows[0], columns[1]) + dot(rows[1], columns[0]) + dot(rows[0], columns[0])
    )


def early_kernel(o, t, o2, u, hi_ref, lo_ref, near_ref, far_ref, squares_ref):
    pts = o.shape[0]
    for i, ref in enumerate((o, t, o2, u)):
        at = slice(i * pts, (i + 1) * pts)
        hi_ref[at], lo_ref[at] = split(ref[...])
        squares_ref[at] = squared(ref[...])

    def part(first, last):
        at = slice(first * pts, last * pts)
        return hi_ref[at], lo_ref[at]

    near_ref[...] = product(part(0, 4), part(0, 2))
    far_ref[...] = product(part(3, 4), part(2, 3))


def late_kernel(t2, v, hi, lo, near, far, squares, mine_ref, sib_ref):
    pts = t2.shape[0]

    def part(first, last):
        at = slice(first * pts, last * pts)
        return hi[at], lo[at]

    crossed, beyond = split(t2[...]), split(v[...])
    both = tuple(jnp.concatenate(pair, axis=0) for pair in zip(crossed, beyond))
    here = product(both, part(0, 2))
    over = product(beyond, part(2, 3)), product(both, crossed)
    ahead = product(part(3, 4), crossed)
    sums = [squares[i * pts : (i + 1) * pts] for i in range(4)]
    sums = sums[:3] + [squared(t2[...]), sums[3], squared(v[...])]
    down = [jnp.sum(x, axis=1, keepdims=True) for x in sums]
    across = [jnp.sum(x.T, axis=0, keepdims=True) for x in sums[:4]]

    def near_block(cand, target):
        lanes = slice(target * pts, (target + 1) * pts)
        if cand in (3, 5):
            at = 0 if cand == 3 else pts
            return here[at : at + pts, lanes]
        at = (0, 1, 2, None, 3)[cand] * pts
        return near[at : at + pts, lanes]

    far_block = {
        (4, 2): far[...],
        (5, 2): over[0],
        (5, 3): over[1][pts : 2 * pts],
        (4, 3): ahead,
    }

    def put(ref, at, block, cand, target):
        ref[at * pts : (at + 1) * pts] = down[cand] + across[target] - 2.0 * block

    for i in range(6):
        put(mine_ref, i, near_block(i, 0), i, 0)
        put(sib_ref, i, near_block(i ^ 1, 1), i ^ 1, 1)
    for i in range(2):
        put(mine_ref, 6 + i, far_block[4 + i, 2], 4 + i, 2)
        put(sib_ref, 6 + i, far_block[5 - i, 3], 5 - i, 3)


def exchange_kernel(scale, keep, mine, theirs, floors, across_ref, along_ref):
    pts = mine.shape[1]

    def whole(i):
        at = slice(i * pts, (i + 1) * pts)
        return (mine[at] + theirs[at]) * scale

    def store(ref, blocks):
        tiles = []
        for i, block in blocks:
            tiles += tiles_of(jnp.maximum(block, floors[i * pts : (i + 1) * pts]))
        for i, tile in enumerate(lowest(tiles, keep)):
            ref[i : i + 1] = tile[0:1]

    store(across_ref, ((0, whole(6)), (1, whole(7))))
    store(along_ref, ((2, whole(4).T), (3, whole(6).T)))


def own_kernel(scale, keep, mine, theirs, floors, old, found_ref):
    pts = mine.shape[1]
    tiles = []
    for i in range(6):
        at = slice(i * pts, (i + 1) * pts)
        tiles += tiles_of(jnp.maximum((mine[at] + theirs[at]) * scale, floors[at]))
    for i, tile in enumerate(lowest(tiles, keep)):
        found_ref[i : i + 1] = tile[0:1]
    found_ref[keep : 2 * keep] = old[...]


def finish_kernel(keep, found, across, along, best_ref, total_ref):
    tiles = tiles_of(found[...]) + tiles_of(across[...]) + tiles_of(along[...])
    ranked = lowest(tiles, keep)
    total_ref[...] = jnp.broadcast_to(
        jnp.sum(ranked[keep - 1], axis=1, keepdims=True), total_ref.shape
    )
    for i, tile in enumerate(ranked):
        best_ref[i : i + 1] = tile[0:1]


def body(points, cand_index, cand_count, neighbor_ids, old_dist):
    pts, width = points.shape
    keep = old_dist.shape[1]
    cycle = lax.axis_size("blk")
    members = lax.axis_size("grp")
    half = width // 2
    blk = lax.axis_index("blk")
    grp = lax.axis_index("grp")
    core = blk % 2
    f32 = jnp.float32

    def links(move):
        return [
            (b * members + g, (move(b, g)[0] % cycle) * members + move(b, g)[1])
            for b in range(cycle)
            for g in range(members)
        ]

    sibling = links(lambda b, g: (b ^ 1, g))
    over_same = links(lambda b, g: (b, 1 - g))
    over_cross = links(lambda b, g: (b ^ 1, 1 - g))
    along_same = links(lambda b, g: (b + (2 if b % 2 else -2), g))
    along_cross = links(lambda b, g: (b + (1 if b % 2 else -1), g))
    along_back = [(b, a) for a, b in along_same]

    def send(array, pairs):
        return lax.ppermute(array, AXES, pairs)

    whole_array = pl.BlockSpec(memory_space=pltpu.VMEM)
    scalars = pl.BlockSpec(memory_space=pltpu.SMEM)

    def call(kernel, out_shape, args, flops=0, first=whole_array, limit=4):
        return pl.pallas_call(
            kernel,
            out_shape=out_shape,
            in_specs=[first] + [whole_array] * (len(args) - 1),
            out_specs=jax.tree.map(lambda _: whole_array, out_shape),
            cost_estimate=pl.CostEstimate(
                flops=flops, bytes_accessed=0, transcendentals=0
            ),
            compiler_params=pltpu.CompilerParams(vmem_limit_bytes=limit << 20),
        )(*args)

    def array(rows, lanes=pts, dtype=f32):
        return jax.ShapeDtypeStruct((rows, lanes), dtype)

    meta = call(
        describe_kernel,
        array(keep + SUBLANES, dtype=jnp.int32),
        (cand_count, cand_index, neighbor_ids.T),
        first=scalars,
    )
    o = lax.dynamic_slice(points, (0, core * half), (pts, half))
    later, described = lax.optimization_barrier((points, meta))
    other = lax.dynamic_slice(later, (0, (1 - core) * half), (pts, half))

    o2 = send(o, over_same)
    u = send(o, along_same)
    metas = (
        meta,
        send(described, sibling),
        send(described, over_same),
        send(described, over_cross),
        send(described, along_same),
        send(described, along_cross),
    )
    t2 = send(other, over_cross)
    v = send(other, along_cross)
    t = send(other, sibling)

    ahead = jnp.where(core == 0, 2, -2)
    beside = jnp.where(core == 0, -1, 1)
    steps = (0, 1 - 2 * core, 0, 1 - 2 * core, ahead, beside)
    sides = (grp, grp, 1 - grp, 1 - grp, grp, grp)
    bases = jnp.stack(
        [
            ((blk + step + cycle) % cycle) * members + side
            for step, side in zip(steps, sides)
        ]
    ).astype(jnp.int32)
    own_floor, far_floor = call(
        functools.partial(mask_kernel, keep),
        (array(6 * pts), array(4 * pts)),
        (bases,) + metas,
        flops=1 << 29,
        first=scalars,
    )

    block_flops = 6 * pts * pts * half
    hi, lo, near, far, squares = call(
        early_kernel,
        (
            array(4 * pts, half, jnp.bfloat16),
            array(4 * pts, half, jnp.bfloat16),
            array(4 * pts, 2 * pts),
            array(pts),
            array(4 * pts, LANES),
        ),
        (o, t, o2, u),
        flops=9 * block_flops,
        limit=24,
    )
    t2, v, own_floor, far_floor = lax.optimization_barrier(
        (t2, v, own_floor, far_floor)
    )
    mine, for_sibling = call(
        late_kernel,
        (array(8 * pts),) * 2,
        (t2, v, hi, lo, near, far, squares),
        flops=7 * block_flops,
        limit=24,
    )
    theirs = send(for_sibling, sibling)

    scale = 1.0 / width
    across, along = call(
        functools.partial(exchange_kernel, scale, keep),
        (array(keep),) * 2,
        (mine, theirs, far_floor),
        flops=1 << 28,
    )
    across = send(across, over_same)
    along = send(along, along_back)
    found = call(
        functools.partial(own_kernel, scale, keep),
        array(2 * keep),
        (mine, theirs, own_floor, old_dist.T),
        flops=1 << 29,
    )
    best, total = call(
        functools.partial(finish_kernel, keep),
        (array(keep), array(SUBLANES, LANES)),
        (found, across, along),
        flops=1 << 26,
    )

    devices = cycle * members
    copies = jnp.broadcast_to(total[:1].reshape(1, 1, LANES), (devices, 1, LANES))
    totals = lax.all_to_all(copies, AXES, 0, 0)
    mean_last = jnp.sum(totals[:, 0, 0]) / (pts * devices)
    return (best / mean_last).T


def solution(mesh):
    return jax.shard_map(
        body,
        mesh=mesh,
        in_specs=(
            P(AXES, None),
            P(AXES, None),
            P(AXES),
            P(AXES, None),
            P(AXES, None),
        ),
        out_specs=P(AXES, None),
        check_vma=False,
    )
```

```python
import functools

import jax
import jax.numpy as jnp
from jax import lax
from jax.experimental import pallas as pl
from jax.experimental.pallas import tpu as pltpu
from jax.sharding import PartitionSpec as P


AXES = ("blk", "grp")
LANES = 128
SUBLANES = 8
NT = (((1,), (1,)), ((), ()))
FAR = 1e30
NEVER = -3e38


def exchange(tiles, i, j):
    low, high = jnp.minimum(tiles[i], tiles[j]), jnp.maximum(tiles[i], tiles[j])
    tiles[i], tiles[j] = low, high


def sort_tiles(tiles):
    tiles = list(tiles)
    n = len(tiles)
    p = 1
    while p < n:
        k = p
        while k >= 1:
            for j in range(k % p, n - k, 2 * k):
                for i in range(min(k, n - j - k)):
                    if (i + j) // (2 * p) == (i + j + k) // (2 * p):
                        exchange(tiles, i + j, i + j + k)
            k //= 2
        p *= 2
    return tiles


def bitonic(tiles):
    tiles = list(tiles)
    step = len(tiles) // 2
    while step >= 1:
        for i in range(len(tiles)):
            if not i & step:
                exchange(tiles, i, i + step)
        step //= 2
    return tiles


def merge_lowest(a, b, keep):
    if len(a) + len(b) <= keep:
        return bitonic(a + b[::-1])
    return bitonic([jnp.minimum(x, y) for x, y in zip(a, b[::-1])])


def lowest(tiles, keep):
    group = 1
    while group * 2 <= min(keep, len(tiles)):
        group *= 2
    while len(tiles) % group:
        tiles = tiles + [jnp.full((SUBLANES, LANES), FAR, jnp.float32)]
    lists = [sort_tiles(tiles[i : i + group]) for i in range(0, len(tiles), group)]
    while len(lists) > 1:
        paired = [
            merge_lowest(lists[i], lists[i + 1], keep)
            for i in range(0, len(lists) - 1, 2)
        ]
        if len(lists) % 2:
            rest = lists[-1]
            while len(rest) < len(paired[0]):
                rest = rest + [jnp.full((SUBLANES, LANES), FAR, jnp.float32)]
            paired.append(rest)
        lists = paired
    found = lists[0]
    shift = SUBLANES // 2
    while shift:
        found = merge_lowest(found, [pltpu.roll(t, shift, 0) for t in found], keep)
        shift //= 2
    return found


def tiles_of(array):
    return [array[i : i + SUBLANES] for i in range(0, array.shape[0], SUBLANES)]


def describe_kernel(count_ref, index_ref, lists_ref, meta_ref):
    listed, pts = lists_ref.shape
    slots = index_ref.shape[1]
    meta_ref[0:listed] = lists_ref[...]
    spread = jnp.broadcast_to(index_ref[...].astype(jnp.float32), (pts, slots)).T
    slot = lax.broadcasted_iota(jnp.int32, (slots, pts), 0)
    row = lax.broadcasted_iota(jnp.int32, (slots, pts), 1)
    hit = (spread.astype(jnp.int32) == row) & (slot < count_ref[0])
    live = jnp.max(jnp.where(hit, 1.0, 0.0), axis=0, keepdims=True)
    meta_ref[listed : listed + SUBLANES] = jnp.broadcast_to(
        live.astype(jnp.int32), (SUBLANES, pts)
    )


def mask_kernel(listed, base_ref, o, t, o2, t2, u, v, own_ref, far_ref):
    metas = (o, t, o2, t2, u, v)
    pts = o.shape[1]
    alive = [
        jnp.broadcast_to(m[listed : listed + 1].astype(jnp.float32), (pts, pts)).T > 0.5
        for m in metas
    ]
    row = lax.broadcasted_iota(jnp.int32, (pts, pts), 0)
    lane = lax.broadcasted_iota(jnp.int32, (pts, pts), 1)

    def floor(target, cand):
        ids = row + base_ref[cand] * pts
        lists = metas[target]
        bad = jnp.logical_not(alive[cand])
        for k in range(listed):
            bad = bad | (ids == lists[k : k + 1])
        if target == cand:
            bad = bad | (row == lane)
        return jnp.where(bad, FAR, NEVER)

    for i in range(6):
        own_ref[i * pts : (i + 1) * pts] = floor(0, i)
    for i, (target, cand) in enumerate(((2, 4), (2, 5), (4, 0), (4, 2))):
        far_ref[i * pts : (i + 1) * pts] = floor(target, cand)


def split(x):
    high = x.astype(jnp.bfloat16)
    return high, (x - high.astype(jnp.float32)).astype(jnp.bfloat16)


def squared(x):
    total = x[:, :LANES] * x[:, :LANES]
    for j in range(LANES, x.shape[1], LANES):
        total = total + x[:, j : j + LANES] * x[:, j : j + LANES]
    return total


def product(rows, columns):
    def dot(a, b):
        return lax.dot_general(a, b, NT, preferred_element_type=jnp.float32)

    return (
        dot(rows[0], columns[1]) + dot(rows[1], columns[0]) + dot(rows[0], columns[0])
    )


def early_kernel(o, t, o2, u, hi_ref, lo_ref, near_ref, far_ref, squares_ref):
    pts = o.shape[0]
    for i, ref in enumerate((o, t, o2, u)):
        at = slice(i * pts, (i + 1) * pts)
        hi_ref[at], lo_ref[at] = split(ref[...])
        squares_ref[at] = squared(ref[...])

    def part(first, last):
        at = slice(first * pts, last * pts)
        return hi_ref[at], lo_ref[at]

    near_ref[...] = product(part(0, 4), part(0, 2))
    far_ref[...] = product(part(3, 4), part(2, 3))


def middle_kernel(t2, v, hi, lo, here_ref, over_ref, squares_ref):
    pts, width = t2.shape

    def part(first, last):
        at = slice(first * pts, last * pts)
        return hi[at, :width], lo[at, :width]

    blocks = split(t2[...]), split(v[...])
    late_products(blocks, part, pts, here_ref, over_ref)
    squares_ref[0:pts] = squared(t2[...])
    squares_ref[pts : 2 * pts] = squared(v[...])


def late_products(blocks, part, pts, here_ref, over_ref):
    crossed, beyond = blocks
    both = tuple(jnp.concatenate(pair, axis=0) for pair in zip(crossed, beyond))
    here_ref[...] = product(both, part(0, 2))
    over_ref[0:pts] = product(beyond, part(2, 3))
    over_ref[pts : 2 * pts] = product(beyond, crossed)
    over_ref[2 * pts : 3 * pts] = product(part(3, 4), crossed)


def late_kernel(
    t2, v, hi, lo, near, far, squares, here, over, more, mine_ref, sib_ref, rest, last
):
    pts, width = t2.shape
    start = hi.shape[1] - width

    def part(first, last):
        at = slice(first * pts, last * pts)
        return hi[at, start:], lo[at, start:]

    late_products((split(t2[...]), split(v[...])), part, pts, rest, last)
    sums = [squares[i * pts : (i + 1) * pts] for i in range(4)]
    sums = sums[:3] + [
        more[0:pts] + squared(t2[...]),
        sums[3],
        more[pts : 2 * pts] + squared(v[...]),
    ]
    down = [jnp.sum(x, axis=1, keepdims=True) for x in sums]
    across = [jnp.sum(x.T, axis=0, keepdims=True) for x in sums[:4]]

    def near_block(cand, target):
        lanes = slice(target * pts, (target + 1) * pts)
        if cand in (3, 5):
            at = slice(0, pts) if cand == 3 else slice(pts, 2 * pts)
            return here[at, lanes] + rest[at, lanes]
        at = (0, 1, 2, None, 3)[cand] * pts
        return near[at : at + pts, lanes]

    def far_block(cand, target):
        if (cand, target) == (4, 2):
            return far[...]
        i = ((5, 2), (5, 3), (4, 3)).index((cand, target))
        at = slice(i * pts, (i + 1) * pts)
        return over[at] + last[at]

    def put(ref, at, block, cand, target):
        ref[at * pts : (at + 1) * pts] = down[cand] + across[target] - 2.0 * block

    for i in range(6):
        put(mine_ref, i, near_block(i, 0), i, 0)
        put(sib_ref, i, near_block(i ^ 1, 1), i ^ 1, 1)
    for i in range(2):
        put(mine_ref, 6 + i, far_block(4 + i, 2), 4 + i, 2)
        put(sib_ref, 6 + i, far_block(5 - i, 3), 5 - i, 3)


def exchange_kernel(scale, keep, mine, theirs, floors, across_ref, along_ref):
    pts = mine.shape[1]

    def whole(i):
        at = slice(i * pts, (i + 1) * pts)
        return (mine[at] + theirs[at]) * scale

    def store(ref, blocks):
        tiles = []
        for i, block in blocks:
            tiles += tiles_of(jnp.maximum(block, floors[i * pts : (i + 1) * pts]))
        for i, tile in enumerate(lowest(tiles, keep)):
            ref[i : i + 1] = tile[0:1]

    store(across_ref, ((0, whole(6)), (1, whole(7))))
    store(along_ref, ((2, whole(4).T), (3, whole(6).T)))


def own_kernel(scale, keep, mine, theirs, floors, old, found_ref):
    pts = mine.shape[1]
    tiles = []
    for i in range(6):
        at = slice(i * pts, (i + 1) * pts)
        tiles += tiles_of(jnp.maximum((mine[at] + theirs[at]) * scale, floors[at]))
    for i, tile in enumerate(lowest(tiles, keep)):
        found_ref[i : i + 1] = tile[0:1]
    found_ref[keep : 2 * keep] = old[...]


def finish_kernel(keep, found, across, along, best_ref, total_ref):
    tiles = tiles_of(found[...]) + tiles_of(across[...]) + tiles_of(along[...])
    ranked = lowest(tiles, keep)
    total_ref[...] = jnp.broadcast_to(
        jnp.sum(ranked[keep - 1], axis=1, keepdims=True), total_ref.shape
    )
    for i, tile in enumerate(ranked):
        best_ref[i : i + 1] = tile[0:1]


def scale_kernel(points_in_all, best, totals, out_ref):
    total = jnp.sum(totals[:, 0, :], axis=0, keepdims=True)
    out_ref[...] = best[...] / (total * (1.0 / points_in_all))


def cut_kernel(start_ref, points, out_ref, done):
    start = pl.multiple_of(start_ref[0], LANES)
    copy = pltpu.make_async_copy(
        points.at[:, pl.ds(start, out_ref.shape[1])], out_ref, done
    )
    copy.start()
    copy.wait()


def body(points, cand_index, cand_count, neighbor_ids, old_dist):
    pts, width = points.shape
    keep = old_dist.shape[1]
    cycle = lax.axis_size("blk")
    members = lax.axis_size("grp")
    half = width // 2
    blk = lax.axis_index("blk")
    grp = lax.axis_index("grp")
    core = blk % 2
    f32 = jnp.float32

    def links(move):
        return [
            (b * members + g, (move(b, g)[0] % cycle) * members + move(b, g)[1])
            for b in range(cycle)
            for g in range(members)
        ]

    sibling = links(lambda b, g: (b ^ 1, g))
    over_same = links(lambda b, g: (b, 1 - g))
    over_cross = links(lambda b, g: (b ^ 1, 1 - g))
    along_same = links(lambda b, g: (b + (2 if b % 2 else -2), g))
    along_cross = links(lambda b, g: (b + (1 if b % 2 else -1), g))
    along_back = [(b, a) for a, b in along_same]

    def send(array, pairs):
        return lax.ppermute(array, AXES, pairs)

    whole_array = pl.BlockSpec(memory_space=pltpu.VMEM)
    scalars = pl.BlockSpec(memory_space=pltpu.SMEM)

    def call(
        kernel,
        out_shape,
        args,
        flops=0,
        first=whole_array,
        second=whole_array,
        scratch=(),
        limit=4,
    ):
        specs = [first, second] + [whole_array] * len(args)
        return pl.pallas_call(
            kernel,
            out_shape=out_shape,
            in_specs=specs[: len(args)],
            scratch_shapes=scratch,
            out_specs=jax.tree.map(lambda _: whole_array, out_shape),
            cost_estimate=pl.CostEstimate(
                flops=flops, bytes_accessed=0, transcendentals=0
            ),
            compiler_params=pltpu.CompilerParams(vmem_limit_bytes=limit << 20),
        )(*args)

    def array(rows, lanes=pts, dtype=f32):
        return jax.ShapeDtypeStruct((rows, lanes), dtype)

    meta = call(
        describe_kernel,
        array(keep + SUBLANES, dtype=jnp.int32),
        (cand_count, cand_index, neighbor_ids.T),
        first=scalars,
    )

    def cut(source, start):
        return call(
            cut_kernel,
            pltpu.VMEM((pts, half), f32),
            (
                start.astype(jnp.int32).reshape(1),
                pltpu.with_memory_space_constraint(source, pltpu.HBM),
            ),
            first=scalars,
            second=pl.BlockSpec(memory_space=pltpu.HBM),
            scratch=[pltpu.SemaphoreType.DMA],
        )

    o = cut(points, core * half)
    turn, described = lax.optimization_barrier(((1 - core) * half, meta))
    other = cut(points, turn)

    o2 = send(o, over_same)
    u = send(o, along_same)
    metas = (
        meta,
        send(described, sibling),
        send(described, over_same),
        send(described, over_cross),
        send(described, along_same),
        send(described, along_cross),
    )
    most = half * 3 // 4
    t2 = send(other[:, :most], over_cross)
    v = send(other[:, :most], along_cross)
    t2_rest = send(other[:, most:], over_cross)
    v_rest = send(other[:, most:], along_cross)
    t = send(other, sibling)

    ahead = jnp.where(core == 0, 2, -2)
    beside = jnp.where(core == 0, -1, 1)
    steps = (0, 1 - 2 * core, 0, 1 - 2 * core, ahead, beside)
    sides = (grp, grp, 1 - grp, 1 - grp, grp, grp)
    bases = jnp.stack(
        [
            ((blk + step + cycle) % cycle) * members + side
            for step, side in zip(steps, sides)
        ]
    ).astype(jnp.int32)
    own_floor, far_floor = call(
        functools.partial(mask_kernel, keep),
        (array(6 * pts), array(4 * pts)),
        (bases,) + metas,
        flops=1 << 29,
        first=scalars,
    )

    block_flops = 6 * pts * pts * half
    hi, lo, near, far, squares = call(
        early_kernel,
        (
            array(4 * pts, half, jnp.bfloat16),
            array(4 * pts, half, jnp.bfloat16),
            array(4 * pts, 2 * pts),
            array(pts),
            array(4 * pts, LANES),
        ),
        (o, t, o2, u),
        flops=9 * block_flops,
        limit=24,
    )
    here, over, more = call(
        middle_kernel,
        (array(2 * pts, 2 * pts), array(3 * pts), array(2 * pts, LANES)),
        (t2, v, hi, lo),
        flops=6 * block_flops,
        limit=24,
    )
    t2_rest, v_rest, own_floor, far_floor = lax.optimization_barrier(
        (t2_rest, v_rest, own_floor, far_floor)
    )
    mine, for_sibling = call(
        late_kernel,
        (array(8 * pts),) * 2,
        (t2_rest, v_rest, hi, lo, near, far, squares, here, over, more),
        flops=2 * block_flops,
        scratch=[pltpu.VMEM((2 * pts, 2 * pts), f32), pltpu.VMEM((3 * pts, pts), f32)],
        limit=24,
    )
    theirs = send(for_sibling, sibling)

    scale = 1.0 / width
    across, along = call(
        functools.partial(exchange_kernel, scale, keep),
        (array(keep),) * 2,
        (mine, theirs, far_floor),
        flops=1 << 28,
    )
    across = send(across, over_same)
    along = send(along, along_back)
    found = call(
        functools.partial(own_kernel, scale, keep),
        array(2 * keep),
        (mine, theirs, own_floor, old_dist.T),
        flops=1 << 29,
    )
    best, total = call(
        functools.partial(finish_kernel, keep),
        (array(keep), array(SUBLANES, LANES)),
        (found, across, along),
        flops=1 << 26,
    )

    devices = cycle * members
    copies = jnp.broadcast_to(total[:1].reshape(1, 1, LANES), (devices, 1, LANES))
    totals = lax.all_to_all(copies, AXES, 0, 0)
    scaled = call(
        functools.partial(scale_kernel, pts * devices), array(keep), (best, totals)
    )
    return scaled.T


def solution(mesh):
    return jax.shard_map(
        body,
        mesh=mesh,
        in_specs=(
            P(AXES, None),
            P(AXES, None),
            P(AXES),
            P(AXES, None),
            P(AXES, None),
        ),
        out_specs=P(AXES, None),
        check_vma=False,
    )
```

```python
import functools

import jax
import jax.numpy as jnp
from jax import lax
from jax.experimental import pallas as pl
from jax.experimental.pallas import tpu as pltpu
from jax.sharding import PartitionSpec as P


AXES = ("blk", "grp")
LANES = 128
SUBLANES = 8
NT = (((1,), (1,)), ((), ()))
FAR = 1e30
NEVER = -3e38


def exchange(tiles, i, j):
    low, high = jnp.minimum(tiles[i], tiles[j]), jnp.maximum(tiles[i], tiles[j])
    tiles[i], tiles[j] = low, high


def sort_tiles(tiles):
    tiles = list(tiles)
    n = len(tiles)
    p = 1
    while p < n:
        k = p
        while k >= 1:
            for j in range(k % p, n - k, 2 * k):
                for i in range(min(k, n - j - k)):
                    if (i + j) // (2 * p) == (i + j + k) // (2 * p):
                        exchange(tiles, i + j, i + j + k)
            k //= 2
        p *= 2
    return tiles


def bitonic(tiles):
    tiles = list(tiles)
    step = len(tiles) // 2
    while step >= 1:
        for i in range(len(tiles)):
            if not i & step:
                exchange(tiles, i, i + step)
        step //= 2
    return tiles


def merge_lowest(a, b, keep):
    if len(a) + len(b) <= keep:
        return bitonic(a + b[::-1])
    return bitonic([jnp.minimum(x, y) for x, y in zip(a, b[::-1])])


def lowest(tiles, keep):
    group = 1
    while group * 2 <= min(keep, len(tiles)):
        group *= 2
    while len(tiles) % group:
        tiles = tiles + [jnp.full((SUBLANES, LANES), FAR, jnp.float32)]
    lists = [sort_tiles(tiles[i : i + group]) for i in range(0, len(tiles), group)]
    while len(lists) > 1:
        paired = [
            merge_lowest(lists[i], lists[i + 1], keep)
            for i in range(0, len(lists) - 1, 2)
        ]
        if len(lists) % 2:
            rest = lists[-1]
            while len(rest) < len(paired[0]):
                rest = rest + [jnp.full((SUBLANES, LANES), FAR, jnp.float32)]
            paired.append(rest)
        lists = paired
    found = lists[0]
    shift = SUBLANES // 2
    while shift:
        found = merge_lowest(found, [pltpu.roll(t, shift, 0) for t in found], keep)
        shift //= 2
    return found


def tiles_of(array):
    return [array[i : i + SUBLANES] for i in range(0, array.shape[0], SUBLANES)]


def describe_kernel(count_ref, index_ref, lists_ref, meta_ref):
    listed, pts = lists_ref.shape
    slots = index_ref.shape[1]
    meta_ref[0:listed] = lists_ref[...]
    spread = jnp.broadcast_to(index_ref[...].astype(jnp.float32), (pts, slots)).T
    slot = lax.broadcasted_iota(jnp.int32, (slots, pts), 0)
    row = lax.broadcasted_iota(jnp.int32, (slots, pts), 1)
    hit = (spread.astype(jnp.int32) == row) & (slot < count_ref[0])
    live = jnp.max(jnp.where(hit, 1.0, 0.0), axis=0, keepdims=True)
    meta_ref[listed : listed + SUBLANES] = jnp.broadcast_to(
        live.astype(jnp.int32), (SUBLANES, pts)
    )


def mask_kernel(
    listed, cycle, members, o, t, o2, t2, u, v, own_ref, far_ref
):
    blk, grp = lax.axis_index("blk"), lax.axis_index("grp")
    turned = lax.rem(blk, 2)
    steps = (0, 1 - 2 * turned, 0, 1 - 2 * turned, 2 - 4 * turned, 2 * turned - 1)
    sides = (grp, grp, 1 - grp, 1 - grp, grp, grp)
    base = [
        lax.rem(blk + step + cycle, cycle) * members + side
        for step, side in zip(steps, sides)
    ]
    metas = (o, t, o2, t2, u, v)
    pts = o.shape[1]
    alive = [
        jnp.broadcast_to(m[listed : listed + 1].astype(jnp.float32), (pts, pts)).T > 0.5
        for m in metas
    ]
    row = lax.broadcasted_iota(jnp.int32, (pts, pts), 0)
    lane = lax.broadcasted_iota(jnp.int32, (pts, pts), 1)

    def floor(target, cand):
        ids = row + base[cand] * pts
        lists = metas[target]
        bad = jnp.logical_not(alive[cand])
        for k in range(listed):
            bad = bad | (ids == lists[k : k + 1])
        if target == cand:
            bad = bad | (row == lane)
        return jnp.where(bad, FAR, NEVER)

    for i in range(6):
        own_ref[i * pts : (i + 1) * pts] = floor(0, i)
    for i, (target, cand) in enumerate(((2, 4), (2, 5), (4, 0), (4, 2))):
        far_ref[i * pts : (i + 1) * pts] = floor(target, cand)


def split(x):
    high = x.astype(jnp.bfloat16)
    return high, (x - high.astype(jnp.float32)).astype(jnp.bfloat16)


def squared(x):
    total = x[:, :LANES] * x[:, :LANES]
    for j in range(LANES, x.shape[1], LANES):
        total = total + x[:, j : j + LANES] * x[:, j : j + LANES]
    return total


def product(rows, columns):
    def dot(a, b):
        return lax.dot_general(a, b, NT, preferred_element_type=jnp.float32)

    return (
        dot(rows[0], columns[1]) + dot(rows[1], columns[0]) + dot(rows[0], columns[0])
    )


def lengths(total):
    return (
        jnp.sum(total, axis=1, keepdims=True),
        jnp.sum(total.T, axis=0, keepdims=True),
    )


def early_kernel(o, t, o2, u, hi_ref, lo_ref, squares_ref, mine_ref, sib_ref):
    pts = o.shape[0]
    norms = []
    for i, ref in enumerate((o, t, o2, u)):
        at = slice(i * pts, (i + 1) * pts)
        hi_ref[at], lo_ref[at] = split(ref[...])
        squares_ref[at] = squared(ref[...])
        norms.append(lengths(squares_ref[at]))

    def part(first, last):
        at = slice(first * pts, last * pts)
        return hi_ref[at], lo_ref[at]

    near = product(part(0, 4), part(0, 2))

    def put(ref, at, block, cand, target):
        ref[at * pts : (at + 1) * pts] = (
            norms[cand][0] + norms[target][1] - 2.0 * block
        )

    for i in range(4):
        at = slice(i * pts, (i + 1) * pts)
        put(mine_ref, i, near[at, :pts], i, 0)
        put(sib_ref, (1, 0, 2, 3)[i], near[at, pts:], i, 1)
    put(mine_ref, 4, product(part(3, 4), part(2, 3)), 3, 2)


def late_products(blocks, hi, lo):
    crossed, beyond = blocks
    lanes = tuple(jnp.concatenate(pair, axis=0) for pair in zip(crossed, beyond))
    rows = tuple(jnp.concatenate(pair, axis=0) for pair in zip((hi, lo), beyond))
    return product(rows, lanes)


def middle_kernel(t2, v, hi, lo, partial_ref, squares_ref):
    pts, width = t2.shape
    blocks = split(t2[...]), split(v[...])
    partial_ref[...] = late_products(blocks, hi[:, :width], lo[:, :width])
    squares_ref[0:pts] = squared(t2[...])
    squares_ref[pts : 2 * pts] = squared(v[...])


def late_kernel(t2, v, hi, lo, squares, partial, more, mine_ref, sib_ref):
    pts, width = t2.shape
    start = hi.shape[1] - width
    blocks = split(t2[...]), split(v[...])
    total = partial[...] + late_products(blocks, hi[:, start:], lo[:, start:])
    of_o, of_t, of_o2, of_u = [
        lengths(squares[i * pts : (i + 1) * pts]) for i in range(4)
    ]
    of_t2 = lengths(more[0:pts] + squared(t2[...]))
    of_v = lengths(more[pts : 2 * pts] + squared(v[...]))

    def block(row, lane):
        return total[
            row * pts : (row + 1) * pts, lane * pts : (lane + 1) * pts
        ]

    def put(ref, at, product, cand, target):
        ref[at * pts : (at + 1) * pts] = cand[0] + target[1] - 2.0 * product

    put(mine_ref, 0, block(0, 0).T, of_t2, of_o)
    put(mine_ref, 1, block(0, 1).T, of_v, of_o)
    put(mine_ref, 2, block(2, 1).T, of_v, of_o2)
    put(sib_ref, 0, block(1, 0).T, of_t2, of_t)
    put(sib_ref, 1, block(1, 1).T, of_v, of_t)
    put(sib_ref, 2, block(4, 0), of_v, of_t2)
    put(sib_ref, 3, block(3, 0), of_u, of_t2)


def exchange_kernel(
    scale, keep, mine_early, mine_late, their_late, floors, across_ref, along_ref
):
    pts = floors.shape[1]

    def rows(ref, i):
        return ref[i * pts : (i + 1) * pts]

    def store(ref, blocks):
        tiles = []
        for i, block in blocks:
            tiles += tiles_of(jnp.maximum(block * scale, rows(floors, i)))
        for i, tile in enumerate(lowest(tiles, keep)):
            ref[i : i + 1] = tile[0:1]

    near_u = rows(mine_early, 3) + rows(their_late, 1)
    far_u = rows(mine_early, 4) + rows(their_late, 2)
    far_v = rows(mine_late, 2) + rows(their_late, 3)
    store(across_ref, ((0, far_u), (1, far_v)))
    store(along_ref, ((2, near_u.T), (3, far_u.T)))


def own_kernel(
    scale, keep, mine_early, their_early, mine_late, their_late, floors, old, found_ref
):
    pts = floors.shape[1]

    def rows(ref, i):
        return ref[i * pts : (i + 1) * pts]

    blocks = (
        rows(mine_early, 0) + rows(their_early, 0),
        rows(mine_early, 1) + rows(their_early, 1),
        rows(mine_early, 2) + rows(their_late, 0),
        rows(mine_late, 0) + rows(their_early, 2),
        rows(mine_early, 3) + rows(their_late, 1),
        rows(mine_late, 1) + rows(their_early, 3),
    )
    tiles = []
    for i, block in enumerate(blocks):
        tiles += tiles_of(jnp.maximum(block * scale, rows(floors, i)))
    for i, tile in enumerate(lowest(tiles, keep)):
        found_ref[i : i + 1] = tile[0:1]
    found_ref[keep : 2 * keep] = old[...]


def finish_kernel(keep, found, across, along, best_ref, total_ref):
    tiles = tiles_of(found[...]) + tiles_of(across[...]) + tiles_of(along[...])
    ranked = lowest(tiles, keep)
    total = jnp.sum(ranked[keep - 1][0:1], axis=1, keepdims=True)
    total_ref[...] = jnp.broadcast_to(total[None], total_ref.shape)
    for i, tile in enumerate(ranked):
        best_ref[i : i + 1] = tile[0:1]


def scale_kernel(points_in_all, best, totals, out_ref):
    total = jnp.sum(totals[:, 0, :], axis=0, keepdims=True)
    out_ref[...] = best[...] / (total * (1.0 / points_in_all))


def cut_kernel(turned, pieces, points, *refs):
    *outs, done = refs[-1 - len(pieces) :]
    core = lax.rem(lax.axis_index("blk"), 2)
    side = 1 - core if turned else core
    half = points.shape[1] // 2
    copies = []
    for (offset, count), out in zip(pieces, outs):
        rows, width = out.shape
        tall = rows // count
        start = pl.multiple_of(side * half + offset, LANES)
        for i in range(count):
            at = pl.ds(i * tall, tall)
            copies.append(
                pltpu.make_async_copy(
                    points.at[at, pl.ds(start, width)],
                    out.at[at],
                    done.at[len(copies)],
                )
            )
    for copy in copies:
        copy.start()
    for copy in copies:
        copy.wait()


def body(points, cand_index, cand_count, neighbor_ids, old_dist):
    pts, width = points.shape
    keep = old_dist.shape[1]
    cycle = lax.axis_size("blk")
    members = lax.axis_size("grp")
    half = width // 2
    f32 = jnp.float32

    def links(move):
        return [
            (b * members + g, (move(b, g)[0] % cycle) * members + move(b, g)[1])
            for b in range(cycle)
            for g in range(members)
        ]

    sibling = links(lambda b, g: (b ^ 1, g))
    over_same = links(lambda b, g: (b, 1 - g))
    over_cross = links(lambda b, g: (b ^ 1, 1 - g))
    along_same = links(lambda b, g: (b + (2 if b % 2 else -2), g))
    along_cross = links(lambda b, g: (b + (1 if b % 2 else -1), g))
    along_back = [(b, a) for a, b in along_same]

    def send(array, pairs):
        return lax.ppermute(array, AXES, pairs)

    whole_array = pl.BlockSpec(memory_space=pltpu.VMEM)
    scalars = pl.BlockSpec(memory_space=pltpu.SMEM)

    def call(
        kernel,
        out_shape,
        args,
        flops=0,
        first=whole_array,
        second=whole_array,
        scratch=(),
        limit=4,
    ):
        specs = [first, second] + [whole_array] * len(args)
        return pl.pallas_call(
            kernel,
            out_shape=out_shape,
            in_specs=specs[: len(args)],
            scratch_shapes=scratch,
            out_specs=jax.tree.map(lambda _: whole_array, out_shape),
            cost_estimate=pl.CostEstimate(
                flops=flops, bytes_accessed=0, transcendentals=0
            ),
            compiler_params=pltpu.CompilerParams(vmem_limit_bytes=limit << 20),
        )(*args)

    def array(rows, lanes=pts, dtype=f32):
        return jax.ShapeDtypeStruct((rows, lanes), dtype)

    meta = call(
        describe_kernel,
        array(keep + SUBLANES, dtype=jnp.int32),
        (cand_count, cand_index, neighbor_ids.T),
        first=scalars,
    )

    def cut(turned, pieces, after=()):
        held = pl.BlockSpec(memory_space=pltpu.HBM)
        return call(
            functools.partial(
                cut_kernel, turned, [(at, count) for at, _, count in pieces]
            ),
            [pltpu.VMEM((pts, wide), f32) for _, wide, _ in pieces],
            (pltpu.with_memory_space_constraint(points, pltpu.HBM),) + after,
            first=held,
            scratch=[
                pltpu.SemaphoreType.DMA((sum(count for _, _, count in pieces),))
            ],
        )

    most = half * 3 // 4
    (o,) = cut(False, [(0, half, 8)])
    other, other_most, other_rest = cut(
        True, [(0, half, 4), (0, most, 4), (most, half - most, 2)], (meta,)
    )

    o2 = send(o, over_same)
    u = send(o, along_same)
    metas = (
        meta,
        send(meta, sibling),
        send(meta, over_same),
        send(meta, over_cross),
        send(meta, along_same),
        send(meta, along_cross),
    )
    t2 = send(other_most, over_cross)
    v = send(other_most, along_cross)
    t2_rest = send(other_rest, over_cross)
    v_rest = send(other_rest, along_cross)
    t = send(other, sibling)

    own_floor, far_floor = call(
        functools.partial(mask_kernel, keep, cycle, members),
        (array(6 * pts), array(4 * pts)),
        metas,
        flops=1 << 29,
    )

    block_flops = 6 * pts * pts * half
    hi, lo, squares, mine_early, for_sibling = call(
        early_kernel,
        (
            array(4 * pts, half, jnp.bfloat16),
            array(4 * pts, half, jnp.bfloat16),
            array(4 * pts, LANES),
            array(5 * pts),
            array(4 * pts),
        ),
        (o, t, o2, u),
        flops=9 * block_flops,
        limit=24,
    )
    their_early = send(for_sibling, sibling)
    partial, more = call(
        middle_kernel,
        (array(5 * pts, 2 * pts), array(2 * pts, LANES)),
        (t2, v, hi, lo),
        flops=8 * block_flops,
        limit=24,
    )
    t2_rest, v_rest, their_early, own_floor, far_floor = lax.optimization_barrier(
        (t2_rest, v_rest, their_early, own_floor, far_floor)
    )
    mine_late, for_sibling = call(
        late_kernel,
        (array(3 * pts), array(4 * pts)),
        (t2_rest, v_rest, hi, lo, squares, partial, more),
        flops=2 * block_flops,
        limit=24,
    )
    their_late = send(for_sibling, sibling)

    scale = 1.0 / width
    across, along = call(
        functools.partial(exchange_kernel, scale, keep),
        (array(keep),) * 2,
        (mine_early, mine_late, their_late, far_floor),
        flops=1 << 28,
    )
    across = send(across, over_same)
    along = send(along, along_back)
    found = call(
        functools.partial(own_kernel, scale, keep),
        array(2 * keep),
        (mine_early, their_early, mine_late, their_late, own_floor, old_dist.T),
        flops=1 << 29,
    )
    devices = cycle * members
    best, total = call(
        functools.partial(finish_kernel, keep),
        (array(keep), jax.ShapeDtypeStruct((devices, 1, LANES), f32)),
        (found, across, along),
        flops=1 << 26,
    )
    totals = lax.all_to_all(total, AXES, 0, 0)
    scaled = call(
        functools.partial(scale_kernel, pts * devices), array(keep), (best, totals)
    )
    return scaled.T


def solution(mesh):
    return jax.shard_map(
        body,
        mesh=mesh,
        in_specs=(
            P(AXES, None),
            P(AXES, None),
            P(AXES),
            P(AXES, None),
            P(AXES, None),
        ),
        out_specs=P(AXES, None),
        check_vma=False,
    )
```

```python
import functools

import jax
import jax.numpy as jnp
from jax import lax
from jax.experimental import pallas as pl
from jax.experimental.pallas import tpu as pltpu
from jax.sharding import PartitionSpec as P


AXES = ("blk", "grp")
LANES = 128
SUBLANES = 8
NT = (((1,), (1,)), ((), ()))
FAR = 1e30
NEVER = -3e38


def exchange(tiles, i, j):
    low, high = jnp.minimum(tiles[i], tiles[j]), jnp.maximum(tiles[i], tiles[j])
    tiles[i], tiles[j] = low, high


def sort_tiles(tiles):
    tiles = list(tiles)
    n = len(tiles)
    p = 1
    while p < n:
        k = p
        while k >= 1:
            for j in range(k % p, n - k, 2 * k):
                for i in range(min(k, n - j - k)):
                    if (i + j) // (2 * p) == (i + j + k) // (2 * p):
                        exchange(tiles, i + j, i + j + k)
            k //= 2
        p *= 2
    return tiles


def bitonic(tiles):
    tiles = list(tiles)
    step = len(tiles) // 2
    while step >= 1:
        for i in range(len(tiles)):
            if not i & step:
                exchange(tiles, i, i + step)
        step //= 2
    return tiles


def merge_lowest(a, b, keep):
    if len(a) + len(b) <= keep:
        return bitonic(a + b[::-1])
    return bitonic([jnp.minimum(x, y) for x, y in zip(a, b[::-1])])


def lowest(tiles, keep):
    group = 1
    while group * 2 <= min(keep, len(tiles)):
        group *= 2
    while len(tiles) % group:
        tiles = tiles + [jnp.full((SUBLANES, LANES), FAR, jnp.float32)]
    lists = [sort_tiles(tiles[i : i + group]) for i in range(0, len(tiles), group)]
    while len(lists) > 1:
        paired = [
            merge_lowest(lists[i], lists[i + 1], keep)
            for i in range(0, len(lists) - 1, 2)
        ]
        if len(lists) % 2:
            rest = lists[-1]
            while len(rest) < len(paired[0]):
                rest = rest + [jnp.full((SUBLANES, LANES), FAR, jnp.float32)]
            paired.append(rest)
        lists = paired
    found = lists[0]
    shift = SUBLANES // 2
    while shift:
        found = merge_lowest(found, [pltpu.roll(t, shift, 0) for t in found], keep)
        shift //= 2
    return found


def tiles_of(array):
    return [array[i : i + SUBLANES] for i in range(0, array.shape[0], SUBLANES)]


def describe_kernel(count_ref, index_ref, lists_ref, meta_ref):
    listed, pts = lists_ref.shape
    slots = index_ref.shape[1]
    meta_ref[0:listed] = lists_ref[...]
    spread = jnp.broadcast_to(index_ref[...].astype(jnp.float32), (pts, slots)).T
    slot = lax.broadcasted_iota(jnp.int32, (slots, pts), 0)
    row = lax.broadcasted_iota(jnp.int32, (slots, pts), 1)
    hit = (spread.astype(jnp.int32) == row) & (slot < count_ref[0])
    live = jnp.max(jnp.where(hit, 1.0, 0.0), axis=0, keepdims=True)
    meta_ref[listed : listed + SUBLANES] = jnp.broadcast_to(
        live.astype(jnp.int32), (SUBLANES, pts)
    )


def mask_kernel(
    listed, cycle, members, o, t, o2, t2, u, v, own_ref, far_ref
):
    blk, grp = lax.axis_index("blk"), lax.axis_index("grp")
    turned = lax.rem(blk, 2)
    steps = (0, 1 - 2 * turned, 0, 1 - 2 * turned, 2 - 4 * turned, 2 * turned - 1)
    sides = (grp, grp, 1 - grp, 1 - grp, grp, grp)
    base = [
        lax.rem(blk + step + cycle, cycle) * members + side
        for step, side in zip(steps, sides)
    ]
    metas = (o, t, o2, t2, u, v)
    pts = o.shape[1]
    alive = [
        jnp.broadcast_to(m[listed : listed + 1].astype(jnp.float32), (pts, pts)).T > 0.5
        for m in metas
    ]
    row = lax.broadcasted_iota(jnp.int32, (pts, pts), 0)
    lane = lax.broadcasted_iota(jnp.int32, (pts, pts), 1)

    def floor(target, cand):
        ids = row + base[cand] * pts
        lists = metas[target]
        bad = jnp.logical_not(alive[cand])
        for k in range(listed):
            bad = bad | (ids == lists[k : k + 1])
        if target == cand:
            bad = bad | (row == lane)
        return jnp.where(bad, FAR, NEVER)

    for i in range(6):
        own_ref[i * pts : (i + 1) * pts] = floor(0, i)
    for i, (target, cand) in enumerate(((2, 4), (2, 5), (4, 0), (4, 2))):
        far_ref[i * pts : (i + 1) * pts] = floor(target, cand)


def split(x):
    high = x.astype(jnp.bfloat16)
    return high, (x - high.astype(jnp.float32)).astype(jnp.bfloat16)


def squared(x):
    total = x[:, :LANES] * x[:, :LANES]
    for j in range(LANES, x.shape[1], LANES):
        total = total + x[:, j : j + LANES] * x[:, j : j + LANES]
    return total


def product(rows, columns):
    def dot(a, b):
        return lax.dot_general(a, b, NT, preferred_element_type=jnp.float32)

    return (
        dot(rows[0], columns[1]) + dot(rows[1], columns[0]) + dot(rows[0], columns[0])
    )


def lengths(total):
    return (
        jnp.sum(total, axis=1, keepdims=True),
        jnp.sum(total.T, axis=0, keepdims=True),
    )


def early_kernel(*refs):
    *pieces, hi_ref, lo_ref, squares_ref, mine_ref, sib_ref = refs
    pts = pieces[0].shape[0]
    norms = []
    for i, parts in enumerate((pieces[0:2], pieces[2:3], pieces[3:5], pieces[5:7])):
        at = slice(i * pts, (i + 1) * pts)
        start = 0
        total = None
        for ref in parts:
            lanes = slice(start, start + ref.shape[1])
            hi_ref[at, lanes], lo_ref[at, lanes] = split(ref[...])
            total = squared(ref[...]) if total is None else total + squared(ref[...])
            start += ref.shape[1]
        squares_ref[at] = total
        norms.append(lengths(total))

    def part(first, last):
        at = slice(first * pts, last * pts)
        return hi_ref[at], lo_ref[at]

    near = product(part(0, 4), part(0, 2))

    def put(ref, at, block, cand, target):
        ref[at * pts : (at + 1) * pts] = (
            norms[cand][0] + norms[target][1] - 2.0 * block
        )

    for i in range(4):
        at = slice(i * pts, (i + 1) * pts)
        put(mine_ref, i, near[at, :pts], i, 0)
        put(sib_ref, (1, 0, 2, 3)[i], near[at, pts:], i, 1)
    put(mine_ref, 4, product(part(3, 4), part(2, 3)), 3, 2)


def late_products(blocks, hi, lo):
    crossed, beyond = blocks
    lanes = tuple(jnp.concatenate(pair, axis=0) for pair in zip(crossed, beyond))
    rows = tuple(jnp.concatenate(pair, axis=0) for pair in zip((hi, lo), beyond))
    return product(rows, lanes)


def middle_kernel(t2, v, hi, lo, partial_ref, squares_ref):
    pts, width = t2.shape
    blocks = split(t2[...]), split(v[...])
    partial_ref[...] = late_products(blocks, hi[:, :width], lo[:, :width])
    squares_ref[0:pts] = squared(t2[...])
    squares_ref[pts : 2 * pts] = squared(v[...])


def late_kernel(t2, v, hi, lo, squares, partial, more, mine_ref, sib_ref):
    pts, width = t2.shape
    start = hi.shape[1] - width
    blocks = split(t2[...]), split(v[...])
    total = partial[...] + late_products(blocks, hi[:, start:], lo[:, start:])
    of_o, of_t, of_o2, of_u = [
        lengths(squares[i * pts : (i + 1) * pts]) for i in range(4)
    ]
    of_t2 = lengths(more[0:pts] + squared(t2[...]))
    of_v = lengths(more[pts : 2 * pts] + squared(v[...]))

    def block(row, lane):
        return total[
            row * pts : (row + 1) * pts, lane * pts : (lane + 1) * pts
        ]

    def put(ref, at, product, cand, target):
        ref[at * pts : (at + 1) * pts] = cand[0] + target[1] - 2.0 * product

    put(mine_ref, 0, block(0, 0).T, of_t2, of_o)
    put(mine_ref, 1, block(0, 1).T, of_v, of_o)
    put(mine_ref, 2, block(2, 1).T, of_v, of_o2)
    put(sib_ref, 0, block(1, 0).T, of_t2, of_t)
    put(sib_ref, 1, block(1, 1).T, of_v, of_t)
    put(sib_ref, 2, block(4, 0), of_v, of_t2)
    put(sib_ref, 3, block(3, 0), of_u, of_t2)


def exchange_kernel(
    scale, keep, mine_early, mine_late, their_late, floors, across_ref, along_ref
):
    pts = floors.shape[1]

    def rows(ref, i):
        return ref[i * pts : (i + 1) * pts]

    def store(ref, blocks):
        tiles = []
        for i, block in blocks:
            tiles += tiles_of(jnp.maximum(block * scale, rows(floors, i)))
        for i, tile in enumerate(lowest(tiles, keep)):
            ref[i : i + 1] = tile[0:1]

    near_u = rows(mine_early, 3) + rows(their_late, 1)
    far_u = rows(mine_early, 4) + rows(their_late, 2)
    far_v = rows(mine_late, 2) + rows(their_late, 3)
    store(across_ref, ((0, far_u), (1, far_v)))
    store(along_ref, ((2, near_u.T), (3, far_u.T)))


def own_kernel(
    scale, keep, mine_early, their_early, mine_late, their_late, floors, old, found_ref
):
    pts = floors.shape[1]

    def rows(ref, i):
        return ref[i * pts : (i + 1) * pts]

    blocks = (
        rows(mine_early, 0) + rows(their_early, 0),
        rows(mine_early, 1) + rows(their_early, 1),
        rows(mine_early, 2) + rows(their_late, 0),
        rows(mine_late, 0) + rows(their_early, 2),
        rows(mine_early, 3) + rows(their_late, 1),
        rows(mine_late, 1) + rows(their_early, 3),
    )
    tiles = []
    for i, block in enumerate(blocks):
        tiles += tiles_of(jnp.maximum(block * scale, rows(floors, i)))
    for i, tile in enumerate(lowest(tiles, keep)):
        found_ref[i : i + 1] = tile[0:1]
    found_ref[keep : 2 * keep] = old[...]


def finish_kernel(keep, found, across, along, best_ref, total_ref):
    tiles = tiles_of(found[...]) + tiles_of(across[...]) + tiles_of(along[...])
    ranked = lowest(tiles, keep)
    total = jnp.sum(ranked[keep - 1][0:1], axis=1, keepdims=True)
    total_ref[...] = jnp.broadcast_to(total[None], total_ref.shape)
    for i, tile in enumerate(ranked):
        best_ref[i : i + 1] = tile[0:1]


def scale_kernel(points_in_all, best, totals, out_ref):
    total = jnp.sum(totals[:, 0, :], axis=0, keepdims=True)
    out_ref[...] = best[...] / (total * (1.0 / points_in_all))


def cut_kernel(turned, pieces, points, *refs):
    *outs, done = refs[-1 - len(pieces) :]
    core = lax.rem(lax.axis_index("blk"), 2)
    side = 1 - core if turned else core
    half = points.shape[1] // 2
    copies = []
    for (offset, count), out in zip(pieces, outs):
        rows, width = out.shape
        tall = rows // count
        start = pl.multiple_of(side * half + offset, LANES)
        for i in range(count):
            at = pl.ds(i * tall, tall)
            copies.append(
                pltpu.make_async_copy(
                    points.at[at, pl.ds(start, width)],
                    out.at[at],
                    done.at[len(copies)],
                )
            )
    for copy in copies:
        copy.start()
    for copy in copies:
        copy.wait()


def body(points, cand_index, cand_count, neighbor_ids, old_dist):
    pts, width = points.shape
    keep = old_dist.shape[1]
    cycle = lax.axis_size("blk")
    members = lax.axis_size("grp")
    half = width // 2
    f32 = jnp.float32

    def links(move):
        return [
            (b * members + g, (move(b, g)[0] % cycle) * members + move(b, g)[1])
            for b in range(cycle)
            for g in range(members)
        ]

    sibling = links(lambda b, g: (b ^ 1, g))
    over_same = links(lambda b, g: (b, 1 - g))
    over_cross = links(lambda b, g: (b ^ 1, 1 - g))
    along_same = links(lambda b, g: (b + (2 if b % 2 else -2), g))
    along_cross = links(lambda b, g: (b + (1 if b % 2 else -1), g))
    along_back = [(b, a) for a, b in along_same]

    def send(array, pairs):
        return lax.ppermute(array, AXES, pairs)

    whole_array = pl.BlockSpec(memory_space=pltpu.VMEM)
    scalars = pl.BlockSpec(memory_space=pltpu.SMEM)

    def call(
        kernel,
        out_shape,
        args,
        flops=0,
        first=whole_array,
        second=whole_array,
        scratch=(),
        limit=4,
    ):
        specs = [first, second] + [whole_array] * len(args)
        return pl.pallas_call(
            kernel,
            out_shape=out_shape,
            in_specs=specs[: len(args)],
            scratch_shapes=scratch,
            out_specs=jax.tree.map(lambda _: whole_array, out_shape),
            cost_estimate=pl.CostEstimate(
                flops=flops, bytes_accessed=0, transcendentals=0
            ),
            compiler_params=pltpu.CompilerParams(vmem_limit_bytes=limit << 20),
        )(*args)

    def array(rows, lanes=pts, dtype=f32):
        return jax.ShapeDtypeStruct((rows, lanes), dtype)

    meta = call(
        describe_kernel,
        array(keep + SUBLANES, dtype=jnp.int32),
        (cand_count, cand_index, neighbor_ids.T),
        first=scalars,
    )

    def cut(turned, pieces, after=()):
        held = pl.BlockSpec(memory_space=pltpu.HBM)
        return call(
            functools.partial(
                cut_kernel, turned, [(at, count) for at, _, count in pieces]
            ),
            [pltpu.VMEM((pts, wide), f32) for _, wide, _ in pieces],
            (pltpu.with_memory_space_constraint(points, pltpu.HBM),) + after,
            first=held,
            scratch=[
                pltpu.SemaphoreType.DMA((sum(count for _, _, count in pieces),))
            ],
        )

    lead = half // 4
    most = half * 7 // 8
    (o_lead,) = cut(False, [(0, lead, 1)])
    (o_rest,) = cut(False, [(lead, half - lead, 4)])
    other, other_most, other_rest = cut(
        True, [(0, half, 4), (0, most, 4), (most, half - most, 1)], (meta,)
    )

    o2_lead = send(o_lead, over_same)
    u_lead = send(o_lead, along_same)
    o2_rest = send(o_rest, over_same)
    u_rest = send(o_rest, along_same)
    metas = (
        meta,
        send(meta, sibling),
        send(meta, over_same),
        send(meta, over_cross),
        send(meta, along_same),
        send(meta, along_cross),
    )
    t2 = send(other_most, over_cross)
    v = send(other_most, along_cross)
    t2_rest = send(other_rest, over_cross)
    v_rest = send(other_rest, along_cross)
    t = send(other, sibling)

    own_floor, far_floor = call(
        functools.partial(mask_kernel, keep, cycle, members),
        (array(6 * pts), array(4 * pts)),
        metas,
        flops=1 << 29,
    )

    block_flops = 6 * pts * pts * half
    hi, lo, squares, mine_early, for_sibling = call(
        early_kernel,
        (
            array(4 * pts, half, jnp.bfloat16),
            array(4 * pts, half, jnp.bfloat16),
            array(4 * pts, LANES),
            array(5 * pts),
            array(4 * pts),
        ),
        (o_lead, o_rest, t, o2_lead, o2_rest, u_lead, u_rest),
        flops=9 * block_flops,
        limit=24,
    )
    their_early = send(for_sibling, sibling)
    partial, more = call(
        middle_kernel,
        (array(5 * pts, 2 * pts), array(2 * pts, LANES)),
        (t2, v, hi, lo),
        flops=8 * block_flops,
        limit=24,
    )
    t2_rest, v_rest, their_early, own_floor, far_floor = lax.optimization_barrier(
        (t2_rest, v_rest, their_early, own_floor, far_floor)
    )
    mine_late, for_sibling = call(
        late_kernel,
        (array(3 * pts), array(4 * pts)),
        (t2_rest, v_rest, hi, lo, squares, partial, more),
        flops=2 * block_flops,
        limit=24,
    )
    their_late = send(for_sibling, sibling)

    scale = 1.0 / width
    across, along = call(
        functools.partial(exchange_kernel, scale, keep),
        (array(keep),) * 2,
        (mine_early, mine_late, their_late, far_floor),
        flops=1 << 28,
    )
    across = send(across, over_same)
    along = send(along, along_back)
    found = call(
        functools.partial(own_kernel, scale, keep),
        array(2 * keep),
        (mine_early, their_early, mine_late, their_late, own_floor, old_dist.T),
        flops=1 << 29,
    )
    devices = cycle * members
    best, total = call(
        functools.partial(finish_kernel, keep),
        (array(keep), jax.ShapeDtypeStruct((devices, 1, LANES), f32)),
        (found, across, along),
        flops=1 << 26,
    )
    totals = lax.all_to_all(total, AXES, 0, 0)
    scaled = call(
        functools.partial(scale_kernel, pts * devices), array(keep), (best, totals)
    )
    return scaled.T


def solution(mesh):
    return jax.shard_map(
        body,
        mesh=mesh,
        in_specs=(
            P(AXES, None),
            P(AXES, None),
            P(AXES),
            P(AXES, None),
            P(AXES, None),
        ),
        out_specs=P(AXES, None),
        check_vma=False,
    )
```

```python
import functools

import jax
import jax.numpy as jnp
from jax import lax
from jax.experimental import pallas as pl
from jax.experimental.pallas import tpu as pltpu
from jax.sharding import PartitionSpec as P


AXES = ("blk", "grp")
LANES = 128
SUBLANES = 8
NT = (((1,), (1,)), ((), ()))
FAR = 1e30
NEVER = -3e38


def exchange(tiles, i, j):
    low, high = jnp.minimum(tiles[i], tiles[j]), jnp.maximum(tiles[i], tiles[j])
    tiles[i], tiles[j] = low, high


def sort_tiles(tiles):
    tiles = list(tiles)
    n = len(tiles)
    p = 1
    while p < n:
        k = p
        while k >= 1:
            for j in range(k % p, n - k, 2 * k):
                for i in range(min(k, n - j - k)):
                    if (i + j) // (2 * p) == (i + j + k) // (2 * p):
                        exchange(tiles, i + j, i + j + k)
            k //= 2
        p *= 2
    return tiles


def bitonic(tiles):
    tiles = list(tiles)
    step = len(tiles) // 2
    while step >= 1:
        for i in range(len(tiles)):
            if not i & step:
                exchange(tiles, i, i + step)
        step //= 2
    return tiles


def merge_lowest(a, b, keep):
    if len(a) + len(b) <= keep:
        return bitonic(a + b[::-1])
    return bitonic([jnp.minimum(x, y) for x, y in zip(a, b[::-1])])


def lowest(tiles, keep):
    group = 1
    while group * 2 <= min(keep, len(tiles)):
        group *= 2
    while len(tiles) % group:
        tiles = tiles + [jnp.full((SUBLANES, LANES), FAR, jnp.float32)]
    lists = [sort_tiles(tiles[i : i + group]) for i in range(0, len(tiles), group)]
    while len(lists) > 1:
        paired = [
            merge_lowest(lists[i], lists[i + 1], keep)
            for i in range(0, len(lists) - 1, 2)
        ]
        if len(lists) % 2:
            rest = lists[-1]
            while len(rest) < len(paired[0]):
                rest = rest + [jnp.full((SUBLANES, LANES), FAR, jnp.float32)]
            paired.append(rest)
        lists = paired
    found = lists[0]
    shift = SUBLANES // 2
    while shift:
        found = merge_lowest(found, [pltpu.roll(t, shift, 0) for t in found], keep)
        shift //= 2
    return found


def tiles_of(array):
    return [array[i : i + SUBLANES] for i in range(0, array.shape[0], SUBLANES)]


def describe_kernel(count_ref, index_ref, lists_ref, meta_ref):
    listed, pts = lists_ref.shape
    slots = index_ref.shape[1]
    meta_ref[0:listed] = lists_ref[...]
    spread = jnp.broadcast_to(index_ref[...].astype(jnp.float32), (pts, slots)).T
    slot = lax.broadcasted_iota(jnp.int32, (slots, pts), 0)
    row = lax.broadcasted_iota(jnp.int32, (slots, pts), 1)
    hit = (spread.astype(jnp.int32) == row) & (slot < count_ref[0])
    live = jnp.max(jnp.where(hit, 1.0, 0.0), axis=0, keepdims=True)
    meta_ref[listed : listed + SUBLANES] = jnp.broadcast_to(
        live.astype(jnp.int32), (SUBLANES, pts)
    )


def mask_kernel(
    listed, cycle, members, o, t, o2, t2, u, v, own_ref, far_ref
):
    blk, grp = lax.axis_index("blk"), lax.axis_index("grp")
    turned = lax.rem(blk, 2)
    steps = (0, 1 - 2 * turned, 0, 1 - 2 * turned, 2 - 4 * turned, 2 * turned - 1)
    sides = (grp, grp, 1 - grp, 1 - grp, grp, grp)
    base = [
        lax.rem(blk + step + cycle, cycle) * members + side
        for step, side in zip(steps, sides)
    ]
    metas = (o, t, o2, t2, u, v)
    pts = o.shape[1]
    alive = [
        jnp.broadcast_to(m[listed : listed + 1].astype(jnp.float32), (pts, pts)).T > 0.5
        for m in metas
    ]
    row = lax.broadcasted_iota(jnp.int32, (pts, pts), 0)
    lane = lax.broadcasted_iota(jnp.int32, (pts, pts), 1)

    def floor(target, cand):
        ids = row + base[cand] * pts
        lists = metas[target]
        bad = jnp.logical_not(alive[cand])
        for k in range(listed):
            bad = bad | (ids == lists[k : k + 1])
        if target == cand:
            bad = bad | (row == lane)
        return jnp.where(bad, FAR, NEVER)

    for i in range(6):
        own_ref[i * pts : (i + 1) * pts] = floor(0, i)
    for i, (target, cand) in enumerate(((2, 4), (2, 5), (4, 0), (4, 2))):
        far_ref[i * pts : (i + 1) * pts] = floor(target, cand)


def split(x):
    high = x.astype(jnp.bfloat16)
    return high, (x - high.astype(jnp.float32)).astype(jnp.bfloat16)


def squared(x):
    total = x[:, :LANES] * x[:, :LANES]
    for j in range(LANES, x.shape[1], LANES):
        total = total + x[:, j : j + LANES] * x[:, j : j + LANES]
    return total


def product(rows, columns):
    def dot(a, b):
        return lax.dot_general(a, b, NT, preferred_element_type=jnp.float32)

    return (
        dot(rows[0], columns[1]) + dot(rows[1], columns[0]) + dot(rows[0], columns[0])
    )


def lengths(total):
    return (
        jnp.sum(total, axis=1, keepdims=True),
        jnp.sum(total.T, axis=0, keepdims=True),
    )


def add(before, values):
    return [value + ref for value, ref in zip(values, before)] if before else values


def home_kernel(*refs):
    *own, beside, dist_ref, squares_ref = refs
    pts = own[0].shape[0]
    total, squares, start = None, None, 0
    for ref in own:
        lanes = slice(start, start + ref.shape[1])
        start += ref.shape[1]
        here, there = split(ref[...]), split(beside[:, lanes])
        rows = tuple(jnp.concatenate(pair, axis=0) for pair in zip(here, there))
        part = product(rows, here)
        more = [squared(ref[...]), squared(beside[:, lanes])]
        total = part if total is None else total + part
        squares = add(squares, more)
    across = lengths(squares[0])[1]
    for i, sums in enumerate(squares):
        at = slice(i * pts, (i + 1) * pts)
        dist_ref[at] = lengths(sums)[0] + across - 2.0 * total[at]
    squares_ref[...] = squares[0]


def direct_products(o, o2, u, before, hi_ref, lo_ref):
    pts = o.shape[0]
    for i, ref in enumerate((o, o2)):
        at = slice(i * pts, (i + 1) * pts)
        hi_ref[at], lo_ref[at] = split(ref[...])
    ahead = split(u[...])
    rows = [
        jnp.concatenate([ref[pts : 2 * pts], part], axis=0)
        for ref, part in zip((hi_ref, lo_ref), ahead)
    ]
    total = product(rows, (hi_ref[...], lo_ref[...]))
    squares = jnp.concatenate([squared(o2[...]), squared(u[...])], axis=0)
    return add([ref[...] for ref in before], [total, squares])


def passed_products(t2, v, hi, lo, before):
    parts = zip(split(t2[...]), split(v[...]))
    rows = [jnp.concatenate(pair, axis=0) for pair in parts]
    total = product(rows, (hi[...], lo[...]))
    squares = jnp.concatenate([squared(t2[...]), squared(v[...])], axis=0)
    return add([ref[...] for ref in before], [total, squares])


def direct_kernel(o, o2, u, *refs):
    *before, hi_ref, lo_ref, total_ref, squares_ref = refs
    total_ref[...], squares_ref[...] = direct_products(
        o, o2, u, before, hi_ref, lo_ref
    )


def passed_kernel(t2, v, hi, lo, *refs):
    *before, total_ref, squares_ref = refs
    total_ref[...], squares_ref[...] = passed_products(t2, v, hi, lo, before)


def store_lowest(ref, blocks, scale, keep):
    tiles = []
    for block, floor in blocks:
        tiles += tiles_of(jnp.maximum(block * scale, floor))
    for i, tile in enumerate(lowest(tiles, keep)):
        ref[i : i + 1] = tile[0:1]


def last_direct_kernel(scale, keep, o, o2, u, own_squares, floors, *refs):
    *before, hi_ref, lo_ref, squares_ref, dist_ref, along_ref = refs
    pts = o.shape[0]
    total, squares = direct_products(o, o2, u, before, hi_ref, lo_ref)
    squares_ref[...] = squares
    of_o = lengths(own_squares[...])
    of_o2, of_u = lengths(squares[:pts]), lengths(squares[pts:])
    crossed = of_o2[0] + of_o[1] - 2.0 * total[:pts, :pts]
    near = of_u[0] + of_o[1] - 2.0 * total[pts:, :pts]
    far = of_u[0] + of_o2[1] - 2.0 * total[pts:, pts:]
    for i, block in enumerate((crossed, near, far)):
        dist_ref[i * pts : (i + 1) * pts] = block
    pairs = ((near.T, floors[2 * pts : 3 * pts]), (far.T, floors[3 * pts : 4 * pts]))
    store_lowest(along_ref, pairs, scale, keep)


def last_passed_kernel(
    scale, keep, t2, v, hi, lo, own_squares, squares, dist, floors, *refs
):
    *before, dist_ref, across_ref = refs
    pts = t2.shape[0]
    total, passed = passed_products(t2, v, hi, lo, before)
    of_o = lengths(own_squares[...])
    of_o2 = lengths(squares[0:pts])
    of_t2, of_v = lengths(passed[:pts]), lengths(passed[pts:])
    dist_ref[0:pts] = of_t2[0] + of_o[1] - 2.0 * total[:pts, :pts]
    dist_ref[pts : 2 * pts] = of_v[0] + of_o[1] - 2.0 * total[pts:, :pts]
    far = of_v[0] + of_o2[1] - 2.0 * total[pts:, pts:]
    pairs = ((dist[2 * pts : 3 * pts], floors[0:pts]), (far, floors[pts : 2 * pts]))
    store_lowest(across_ref, pairs, scale, keep)


def own_kernel(scale, keep, home, direct, passed, floors, old, found_ref):
    pts = floors.shape[1]
    order = (home, 0), (home, 1), (direct, 0), (passed, 0), (direct, 1), (passed, 1)
    pairs = [
        (ref[at * pts : (at + 1) * pts], floors[i * pts : (i + 1) * pts])
        for i, (ref, at) in enumerate(order)
    ]
    store_lowest(found_ref, pairs, scale, keep)
    found_ref[keep : 2 * keep] = old[...]


def finish_kernel(keep, found, across, along, best_ref, total_ref):
    tiles = tiles_of(found[...]) + tiles_of(across[...]) + tiles_of(along[...])
    ranked = lowest(tiles, keep)
    total = jnp.sum(ranked[keep - 1][0:1], axis=1, keepdims=True)
    total_ref[...] = jnp.broadcast_to(total[None], total_ref.shape)
    for i, tile in enumerate(ranked):
        best_ref[i : i + 1] = tile[0:1]


def scale_kernel(points_in_all, best, totals, out_ref):
    total = jnp.sum(totals[:, 0, :], axis=0, keepdims=True)
    out_ref[...] = best[...] / (total * (1.0 / points_in_all))


def cut_kernel(spans, points, *refs):
    *outs, done = refs[-1 - len(spans) :]
    copies = [
        pltpu.make_async_copy(points.at[:, pl.ds(start, width)], out, done.at[i])
        for i, ((start, width), out) in enumerate(zip(spans, outs))
    ]
    for copy in copies:
        copy.start()
    for copy in copies:
        copy.wait()


CUTS = (0, 2, 8, 13, 15, 16)


def body(points, cand_index, cand_count, neighbor_ids, old_dist):
    pts, width = points.shape
    keep = old_dist.shape[1]
    cycle = lax.axis_size("blk")
    members = lax.axis_size("grp")
    f32 = jnp.float32

    def links(move):
        return [
            (b * members + g, (move(b, g)[0] % cycle) * members + move(b, g)[1])
            for b in range(cycle)
            for g in range(members)
        ]

    sibling = links(lambda b, g: (b ^ 1, g))
    over_same = links(lambda b, g: (b, 1 - g))
    over_cross = links(lambda b, g: (b ^ 1, 1 - g))
    along_same = links(lambda b, g: (b + (2 if b % 2 else -2), g))
    along_cross = links(lambda b, g: (b + (1 if b % 2 else -1), g))
    along_back = [(b, a) for a, b in along_same]

    def labelled(value, pairs):
        return lax.ppermute(value, AXES, pairs)

    whole_array = pl.BlockSpec(memory_space=pltpu.VMEM)
    scalars = pl.BlockSpec(memory_space=pltpu.SMEM)

    def call(
        kernel,
        out_shape,
        args,
        flops=0,
        first=whole_array,
        second=whole_array,
        scratch=(),
        limit=4,
    ):
        specs = [first, second] + [whole_array] * len(args)
        return pl.pallas_call(
            kernel,
            out_shape=out_shape,
            in_specs=specs[: len(args)],
            scratch_shapes=scratch,
            out_specs=jax.tree.map(lambda _: whole_array, out_shape),
            cost_estimate=pl.CostEstimate(
                flops=flops, bytes_accessed=0, transcendentals=0
            ),
            compiler_params=pltpu.CompilerParams(vmem_limit_bytes=limit << 20),
        )(*args)

    def array(rows, lanes=pts, dtype=f32):
        return jax.ShapeDtypeStruct((rows, lanes), dtype)

    def cut(pieces, after=()):
        return call(
            functools.partial(cut_kernel, pieces),
            [pltpu.VMEM((pts, wide), f32) for _, wide in pieces],
            (pltpu.with_memory_space_constraint(points, pltpu.HBM),) + after,
            first=pl.BlockSpec(memory_space=pltpu.HBM),
            scratch=[pltpu.SemaphoreType.DMA((len(pieces),))],
        )

    meta = call(
        describe_kernel,
        array(keep + SUBLANES, dtype=jnp.int32),
        (cand_count, cand_index, neighbor_ids.T),
        first=scalars,
    )
    cuts = [width * c // CUTS[-1] for c in CUTS]
    spans = [(a, b - a) for a, b in zip(cuts, cuts[1:])]
    o = cut(spans[:1])
    o += cut(spans[1:2])
    o += cut(spans[2:], (meta,))
    metas = (
        meta,
        labelled(meta, sibling),
        labelled(meta, over_same),
        labelled(meta, over_cross),
        labelled(meta, along_same),
        labelled(meta, along_cross),
    )
    u = [labelled(piece, along_same) for piece in o]
    o2 = [labelled(piece, over_same) for piece in o]
    t = labelled(points, sibling)
    t2 = [labelled(piece, sibling) for piece in o2]
    v = [labelled(piece, sibling) for piece in u]

    own_floor, far_floor = call(
        functools.partial(mask_kernel, keep, cycle, members),
        (array(6 * pts), array(4 * pts)),
        metas,
        flops=1 << 29,
    )
    block_flops = 6 * pts * pts * width
    home, own_squares = call(
        home_kernel,
        (array(2 * pts), array(pts, LANES)),
        (*o, t),
        flops=2 * block_flops,
        limit=24,
    )

    scale = 1.0 / width
    final = len(spans) - 1
    direct, passed = (), ()
    for i, (_, wide) in enumerate(spans):
        parts = (array(2 * pts, wide, jnp.bfloat16),) * 2
        sums = (array(2 * pts, 2 * pts), array(2 * pts, LANES))
        flops = 4 * block_flops * wide // width
        if i < final:
            hi, lo, *direct = call(
                direct_kernel,
                parts + sums,
                (o[i], o2[i], u[i], *direct),
                flops=flops,
                limit=16,
            )
            passed = call(
                passed_kernel,
                sums,
                (t2[i], v[i], hi, lo, *passed),
                flops=flops,
                limit=16,
            )
    ready = (o2[final], u[final], own_squares, own_floor, far_floor)
    o2_last, u_last, own_squares, own_floor, far_floor = lax.optimization_barrier(ready)
    hi, lo, squares, direct_dist, along = call(
        functools.partial(last_direct_kernel, scale, keep),
        parts + (array(2 * pts, LANES), array(3 * pts), array(keep)),
        (o[final], o2_last, u_last, own_squares, far_floor, *direct),
        flops=flops,
        limit=16,
    )
    along = labelled(along, along_back)
    passed_dist, across = call(
        functools.partial(last_passed_kernel, scale, keep),
        (array(2 * pts), array(keep)),
        (t2[final], v[final], hi, lo)
        + (own_squares, squares, direct_dist, far_floor, *passed),
        flops=flops,
        limit=16,
    )
    across = labelled(across, over_same)
    found = call(
        functools.partial(own_kernel, scale, keep),
        array(2 * keep),
        (home, direct_dist, passed_dist, own_floor, old_dist.T),
        flops=1 << 29,
    )
    devices = cycle * members
    best, total = call(
        functools.partial(finish_kernel, keep),
        (array(keep), jax.ShapeDtypeStruct((devices, 1, LANES), f32)),
        (found, across, along),
        flops=1 << 26,
    )
    totals = lax.all_to_all(total, AXES, 0, 0)
    scaled = call(
        functools.partial(scale_kernel, pts * devices), array(keep), (best, totals)
    )
    return scaled.T


def solution(mesh):
    return jax.shard_map(
        body,
        mesh=mesh,
        in_specs=(
            P(AXES, None),
            P(AXES, None),
            P(AXES),
            P(AXES, None),
            P(AXES, None),
        ),
        out_specs=P(AXES, None),
        check_vma=False,
    )
```

```python
import functools

import jax
import jax.numpy as jnp
from jax import lax
from jax.experimental import pallas as pl
from jax.experimental.pallas import tpu as pltpu
from jax.sharding import PartitionSpec as P


AXES = ("blk", "grp")
LANES = 128
SUBLANES = 8
NT = (((1,), (1,)), ((), ()))
FAR = 1e30
NEVER = -3e38


def exchange(tiles, i, j):
    low, high = jnp.minimum(tiles[i], tiles[j]), jnp.maximum(tiles[i], tiles[j])
    tiles[i], tiles[j] = low, high


def sort_tiles(tiles):
    tiles = list(tiles)
    n = len(tiles)
    p = 1
    while p < n:
        k = p
        while k >= 1:
            for j in range(k % p, n - k, 2 * k):
                for i in range(min(k, n - j - k)):
                    if (i + j) // (2 * p) == (i + j + k) // (2 * p):
                        exchange(tiles, i + j, i + j + k)
            k //= 2
        p *= 2
    return tiles


def bitonic(tiles):
    tiles = list(tiles)
    step = len(tiles) // 2
    while step >= 1:
        for i in range(len(tiles)):
            if not i & step:
                exchange(tiles, i, i + step)
        step //= 2
    return tiles


def merge_lowest(a, b, keep):
    if len(a) + len(b) <= keep:
        return bitonic(a + b[::-1])
    return bitonic([jnp.minimum(x, y) for x, y in zip(a, b[::-1])])


def lowest(tiles, keep):
    group = 1
    while group * 2 <= min(keep, len(tiles)):
        group *= 2
    while len(tiles) % group:
        tiles = tiles + [jnp.full((SUBLANES, LANES), FAR, jnp.float32)]
    lists = [sort_tiles(tiles[i : i + group]) for i in range(0, len(tiles), group)]
    while len(lists) > 1:
        paired = [
            merge_lowest(lists[i], lists[i + 1], keep)
            for i in range(0, len(lists) - 1, 2)
        ]
        if len(lists) % 2:
            rest = lists[-1]
            while len(rest) < len(paired[0]):
                rest = rest + [jnp.full((SUBLANES, LANES), FAR, jnp.float32)]
            paired.append(rest)
        lists = paired
    found = lists[0]
    shift = SUBLANES // 2
    while shift:
        found = merge_lowest(found, [pltpu.roll(t, shift, 0) for t in found], keep)
        shift //= 2
    return found


def tiles_of(array):
    return [array[i : i + SUBLANES] for i in range(0, array.shape[0], SUBLANES)]


def describe_kernel(count_ref, index_ref, lists_ref, meta_ref):
    listed, pts = lists_ref.shape
    slots = index_ref.shape[1]
    meta_ref[0:listed] = lists_ref[...]
    spread = jnp.broadcast_to(index_ref[...].astype(jnp.float32), (pts, slots)).T
    slot = lax.broadcasted_iota(jnp.int32, (slots, pts), 0)
    row = lax.broadcasted_iota(jnp.int32, (slots, pts), 1)
    hit = (spread.astype(jnp.int32) == row) & (slot < count_ref[0])
    live = jnp.max(jnp.where(hit, 1.0, 0.0), axis=0, keepdims=True)
    meta_ref[listed : listed + SUBLANES] = jnp.broadcast_to(
        live.astype(jnp.int32), (SUBLANES, pts)
    )


def mask_kernel(
    listed, cycle, members, o, t, o2, t2, u, v, own_ref, far_ref
):
    blk, grp = lax.axis_index("blk"), lax.axis_index("grp")
    turned = lax.rem(blk, 2)
    steps = (0, 1 - 2 * turned, 0, 1 - 2 * turned, 2 - 4 * turned, 2 * turned - 1)
    sides = (grp, grp, 1 - grp, 1 - grp, grp, grp)
    base = [
        lax.rem(blk + step + cycle, cycle) * members + side
        for step, side in zip(steps, sides)
    ]
    metas = (o, t, o2, t2, u, v)
    pts = o.shape[1]
    alive = [
        jnp.broadcast_to(m[listed : listed + 1].astype(jnp.float32), (pts, pts)).T > 0.5
        for m in metas
    ]
    row = lax.broadcasted_iota(jnp.int32, (pts, pts), 0)
    lane = lax.broadcasted_iota(jnp.int32, (pts, pts), 1)

    def floor(target, cand):
        ids = row + base[cand] * pts
        lists = metas[target]
        bad = jnp.logical_not(alive[cand])
        for k in range(listed):
            bad = bad | (ids == lists[k : k + 1])
        if target == cand:
            bad = bad | (row == lane)
        return jnp.where(bad, FAR, NEVER)

    for i in range(6):
        own_ref[i * pts : (i + 1) * pts] = floor(0, i)
    for i, (target, cand) in enumerate(((2, 4), (2, 5), (4, 0), (4, 2))):
        far_ref[i * pts : (i + 1) * pts] = floor(target, cand)


def split(x):
    high = x.astype(jnp.bfloat16)
    return high, (x - high.astype(jnp.float32)).astype(jnp.bfloat16)


def squared(x):
    total = x[:, :LANES] * x[:, :LANES]
    for j in range(LANES, x.shape[1], LANES):
        total = total + x[:, j : j + LANES] * x[:, j : j + LANES]
    return total


def product(rows, columns):
    def dot(a, b):
        return lax.dot_general(a, b, NT, preferred_element_type=jnp.float32)

    return (
        dot(rows[0], columns[1]) + dot(rows[1], columns[0]) + dot(rows[0], columns[0])
    )


def lengths(total):
    return (
        jnp.sum(total, axis=1, keepdims=True),
        jnp.sum(total.T, axis=0, keepdims=True),
    )


def add(before, values):
    return [value + ref for value, ref in zip(values, before)] if before else values


def home_kernel(*refs):
    *own, beside, dist_ref, squares_ref = refs
    pts = own[0].shape[0]
    total, squares, start = None, None, 0
    for ref in own:
        lanes = slice(start, start + ref.shape[1])
        start += ref.shape[1]
        here, there = split(ref[...]), split(beside[:, lanes])
        rows = tuple(jnp.concatenate(pair, axis=0) for pair in zip(here, there))
        part = product(rows, here)
        more = [squared(ref[...]), squared(beside[:, lanes])]
        total = part if total is None else total + part
        squares = add(squares, more)
    across = lengths(squares[0])[1]
    for i, sums in enumerate(squares):
        at = slice(i * pts, (i + 1) * pts)
        dist_ref[at] = lengths(sums)[0] + across - 2.0 * total[at]
    squares_ref[...] = squares[0]


def direct_products(o, o2, u, before, hi_ref, lo_ref):
    pts = o.shape[0]
    for i, ref in enumerate((o, o2)):
        at = slice(i * pts, (i + 1) * pts)
        hi_ref[at], lo_ref[at] = split(ref[...])
    ahead = split(u[...])
    rows = [
        jnp.concatenate([ref[pts : 2 * pts], part], axis=0)
        for ref, part in zip((hi_ref, lo_ref), ahead)
    ]
    total = product(rows, (hi_ref[...], lo_ref[...]))
    squares = jnp.concatenate([squared(o2[...]), squared(u[...])], axis=0)
    return add([ref[...] for ref in before], [total, squares])


def passed_products(t2, v, hi, lo, before):
    parts = zip(split(t2[...]), split(v[...]))
    rows = [jnp.concatenate(pair, axis=0) for pair in parts]
    total = product(rows, (hi[...], lo[...]))
    squares = jnp.concatenate([squared(t2[...]), squared(v[...])], axis=0)
    return add([ref[...] for ref in before], [total, squares])


def direct_kernel(o, o2, u, *refs):
    *before, hi_ref, lo_ref, total_ref, squares_ref = refs
    total_ref[...], squares_ref[...] = direct_products(
        o, o2, u, before, hi_ref, lo_ref
    )


def passed_kernel(t2, v, hi, lo, *refs):
    *before, total_ref, squares_ref = refs
    total_ref[...], squares_ref[...] = passed_products(t2, v, hi, lo, before)


def store_lowest(ref, blocks, scale, keep):
    tiles = []
    for block, floor in blocks:
        tiles += tiles_of(jnp.maximum(block * scale, floor))
    for i, tile in enumerate(lowest(tiles, keep)):
        ref[i : i + 1] = tile[0:1]


def last_direct_kernel(scale, keep, o, o2, u, own_squares, floors, *refs):
    *before, hi_ref, lo_ref, squares_ref, dist_ref, along_ref = refs
    pts = o.shape[0]
    total, squares = direct_products(o, o2, u, before, hi_ref, lo_ref)
    squares_ref[...] = squares
    of_o = lengths(own_squares[...])
    of_o2, of_u = lengths(squares[:pts]), lengths(squares[pts:])
    crossed = of_o2[0] + of_o[1] - 2.0 * total[:pts, :pts]
    near = of_u[0] + of_o[1] - 2.0 * total[pts:, :pts]
    far = of_u[0] + of_o2[1] - 2.0 * total[pts:, pts:]
    for i, block in enumerate((crossed, near, far)):
        dist_ref[i * pts : (i + 1) * pts] = block
    pairs = ((near.T, floors[2 * pts : 3 * pts]), (far.T, floors[3 * pts : 4 * pts]))
    store_lowest(along_ref, pairs, scale, keep)


def last_passed_kernel(
    scale, keep, t2, v, hi, lo, own_squares, squares, dist, floors, *refs
):
    *before, dist_ref, across_ref = refs
    pts = t2.shape[0]
    total, passed = passed_products(t2, v, hi, lo, before)
    of_o = lengths(own_squares[...])
    of_o2 = lengths(squares[0:pts])
    of_t2, of_v = lengths(passed[:pts]), lengths(passed[pts:])
    dist_ref[0:pts] = of_t2[0] + of_o[1] - 2.0 * total[:pts, :pts]
    dist_ref[pts : 2 * pts] = of_v[0] + of_o[1] - 2.0 * total[pts:, :pts]
    far = of_v[0] + of_o2[1] - 2.0 * total[pts:, pts:]
    pairs = ((dist[2 * pts : 3 * pts], floors[0:pts]), (far, floors[pts : 2 * pts]))
    store_lowest(across_ref, pairs, scale, keep)


def own_kernel(scale, keep, home, direct, passed, floors, old, found_ref):
    pts = floors.shape[1]
    order = (home, 0), (home, 1), (direct, 0), (passed, 0), (direct, 1), (passed, 1)
    pairs = [
        (ref[at * pts : (at + 1) * pts], floors[i * pts : (i + 1) * pts])
        for i, (ref, at) in enumerate(order)
    ]
    store_lowest(found_ref, pairs, scale, keep)
    found_ref[keep : 2 * keep] = old[...]


def finish_kernel(keep, found, across, along, best_ref, total_ref):
    tiles = tiles_of(found[...]) + tiles_of(across[...]) + tiles_of(along[...])
    ranked = lowest(tiles, keep)
    total = jnp.sum(ranked[keep - 1][0:1], axis=1, keepdims=True)
    total_ref[...] = jnp.broadcast_to(total[None], total_ref.shape)
    for i, tile in enumerate(ranked):
        best_ref[i : i + 1] = tile[0:1]


def scale_kernel(points_in_all, best, totals, out_ref):
    total = jnp.sum(totals[:, 0, :], axis=0, keepdims=True)
    out_ref[...] = best[...] / (total * (1.0 / points_in_all))


def cut_kernel(spans, points, *refs):
    *outs, done = refs[-1 - len(spans) :]
    copies = [
        pltpu.make_async_copy(points.at[:, pl.ds(start, width)], out, done.at[i])
        for i, ((start, width), out) in enumerate(zip(spans, outs))
    ]
    for copy in copies:
        copy.start()
    for copy in copies:
        copy.wait()


CUTS = (0, 4, 8, 13, 16)


def body(points, cand_index, cand_count, neighbor_ids, old_dist):
    pts, width = points.shape
    keep = old_dist.shape[1]
    cycle = lax.axis_size("blk")
    members = lax.axis_size("grp")
    f32 = jnp.float32

    def links(move):
        return [
            (b * members + g, (move(b, g)[0] % cycle) * members + move(b, g)[1])
            for b in range(cycle)
            for g in range(members)
        ]

    sibling = links(lambda b, g: (b ^ 1, g))
    over_same = links(lambda b, g: (b, 1 - g))
    over_cross = links(lambda b, g: (b ^ 1, 1 - g))
    along_same = links(lambda b, g: (b + (2 if b % 2 else -2), g))
    along_cross = links(lambda b, g: (b + (1 if b % 2 else -1), g))
    along_back = [(b, a) for a, b in along_same]

    def labelled(value, pairs):
        return lax.ppermute(value, AXES, pairs)

    whole_array = pl.BlockSpec(memory_space=pltpu.VMEM)
    scalars = pl.BlockSpec(memory_space=pltpu.SMEM)

    def call(
        kernel,
        out_shape,
        args,
        flops=0,
        first=whole_array,
        second=whole_array,
        scratch=(),
        limit=4,
    ):
        specs = [first, second] + [whole_array] * len(args)
        return pl.pallas_call(
            kernel,
            out_shape=out_shape,
            in_specs=specs[: len(args)],
            scratch_shapes=scratch,
            out_specs=jax.tree.map(lambda _: whole_array, out_shape),
            cost_estimate=pl.CostEstimate(
                flops=flops, bytes_accessed=0, transcendentals=0
            ),
            compiler_params=pltpu.CompilerParams(vmem_limit_bytes=limit << 20),
        )(*args)

    def array(rows, lanes=pts, dtype=f32):
        return jax.ShapeDtypeStruct((rows, lanes), dtype)

    def cut(pieces, after=()):
        return call(
            functools.partial(cut_kernel, pieces),
            [pltpu.VMEM((pts, wide), f32) for _, wide in pieces],
            (pltpu.with_memory_space_constraint(points, pltpu.HBM),) + after,
            first=pl.BlockSpec(memory_space=pltpu.HBM),
            scratch=[pltpu.SemaphoreType.DMA((len(pieces),))],
        )

    meta = call(
        describe_kernel,
        array(keep + SUBLANES, dtype=jnp.int32),
        (cand_count, cand_index, neighbor_ids.T),
        first=scalars,
    )
    cuts = [width * c // CUTS[-1] for c in CUTS]
    spans = [(a, b - a) for a, b in zip(cuts, cuts[1:])]
    o = cut(spans[:1])
    o += cut(spans[1:], (meta,))
    metas = (
        meta,
        labelled(meta, sibling),
        labelled(meta, over_same),
        labelled(meta, over_cross),
        labelled(meta, along_same),
        labelled(meta, along_cross),
    )
    u = [labelled(piece, along_same) for piece in o]
    o2 = [labelled(piece, over_same) for piece in o]
    t = labelled(points, sibling)
    t2 = [labelled(piece, sibling) for piece in o2]
    v = [labelled(piece, sibling) for piece in u]

    own_floor, far_floor = call(
        functools.partial(mask_kernel, keep, cycle, members),
        (array(6 * pts), array(4 * pts)),
        metas,
        flops=1 << 29,
    )
    block_flops = 6 * pts * pts * width
    home, own_squares = call(
        home_kernel,
        (array(2 * pts), array(pts, LANES)),
        (*o, t),
        flops=2 * block_flops,
        limit=24,
    )

    scale = 1.0 / width
    final = len(spans) - 1
    direct, passed = (), ()
    for i, (_, wide) in enumerate(spans):
        parts = (array(2 * pts, wide, jnp.bfloat16),) * 2
        sums = (array(2 * pts, 2 * pts), array(2 * pts, LANES))
        flops = 4 * block_flops * wide // width
        if i < final:
            hi, lo, *direct = call(
                direct_kernel,
                parts + sums,
                (o[i], o2[i], u[i], *direct),
                flops=flops,
                limit=16,
            )
            passed = call(
                passed_kernel,
                sums,
                (t2[i], v[i], hi, lo, *passed),
                flops=flops,
                limit=16,
            )
    ready = (o2[final], u[final], own_squares, own_floor, far_floor)
    o2_last, u_last, own_squares, own_floor, far_floor = lax.optimization_barrier(ready)
    hi, lo, squares, direct_dist, along = call(
        functools.partial(last_direct_kernel, scale, keep),
        parts + (array(2 * pts, LANES), array(3 * pts), array(keep)),
        (o[final], o2_last, u_last, own_squares, far_floor, *direct),
        flops=flops,
        limit=16,
    )
    along = labelled(along, along_back)
    passed_dist, across = call(
        functools.partial(last_passed_kernel, scale, keep),
        (array(2 * pts), array(keep)),
        (t2[final], v[final], hi, lo)
        + (own_squares, squares, direct_dist, far_floor, *passed),
        flops=flops,
        limit=16,
    )
    across = labelled(across, over_same)
    found = call(
        functools.partial(own_kernel, scale, keep),
        array(2 * keep),
        (home, direct_dist, passed_dist, own_floor, old_dist.T),
        flops=1 << 29,
    )
    devices = cycle * members
    best, total = call(
        functools.partial(finish_kernel, keep),
        (array(keep), jax.ShapeDtypeStruct((devices, 1, LANES), f32)),
        (found, across, along),
        flops=1 << 26,
    )
    totals = lax.all_to_all(total, AXES, 0, 0)
    scaled = call(
        functools.partial(scale_kernel, pts * devices), array(keep), (best, totals)
    )
    return scaled.T


def solution(mesh):
    return jax.shard_map(
        body,
        mesh=mesh,
        in_specs=(
            P(AXES, None),
            P(AXES, None),
            P(AXES),
            P(AXES, None),
            P(AXES, None),
        ),
        out_specs=P(AXES, None),
        check_vma=False,
    )
```
